256 devices in a mesh: chan: 32 (over y, z_lo, core), slot: 8 (over z_hi, x).
Axes of the slice: x: 4, y: 4, z: 8 (z_hi: 2, z_lo: 4; z = z_hi * 4 + z_lo), core: 2. Of those that a mesh axis runs over, the one named last changes fastest.
Arguments:
- measured_real: float32 [8, 32, 1770], P('slot', 'chan'), may hold values from -60 to 60
- measured_imaginary: float32 [8, 32, 1770], P('slot', 'chan'), may hold values from -60 to 60
- measured_weight: float32 [8, 32, 1770], P('slot', 'chan'), may hold values from 0.3 to 3
- baseline_vectors: float32 [8, 3, 1770], P('slot'), may hold values from -120 to 120
- antenna_pairs: int32 [2, 1770], replicated, may hold values from 0 to 59, as said below
- directions: float32 [3, 200], replicated, may hold values from -0.12 to 0.12
- direction_flux: float32 [32, 200], P('chan'), may hold values from 0.2 to 2
- channel_frequency: float32 [32], P('chan'), may hold values from 1.1 to 1.9
- electron_content_start: float32 [8, 60, 200], P('slot'), may hold values from -6 to 6
- pierce_station_direction: int32 [8, 12000], P('slot'), may hold values from 0 to 11999, each once within a row
- eigen_basis: float32 [12000, 2048], P('chan'), may hold values from -0.0546875 to 0.0546875
- eigen_weight: float32 [2048], replicated, may hold values from 0.1 to 1
Outputs:
- tec_final: float32 [8, 60, 200], P('slot')
- coefficients: float32 [8, 2048], P('slot')
- final_residual_real: float32 [8, 32, 1770], P('slot', 'chan')
- final_residual_imaginary: float32 [8, 32, 1770], P('slot', 'chan')
The draws below stay inside these ranges and needn't reach their ends.
Inputs may be any that keep to these rules, and one draw needn't show every extreme that they name: `antenna_pairs`: each column is a pair of two different stations, and the 1770 columns hold every unordered pair of stations exactly once. `pierce_station_direction`: each row names every station-direction pair exactly once.
All inputs are finite; a program needn't handle non-finite values.
Results may differ from the reference program's by a relative error of at most 0.00018.
Values sent between devices are 32-bit elements; how exact they have to be, the bound alone decides.
No kernel may reach another device: no remote copies, remote signals or barrier semaphores. Data moves between devices by JAX's collectives and lax.ppermute only.
A program may use at most 64 MiB of HBM per device.

```python
import math
import jax
import jax.numpy as jnp
from jax import lax

S = 60
D = 200
K = 2048
ITERS = 4
STATION_PAIRS = 1770
P_SIZE = 12000
TIME_SLOTS = 8
FREQ_CHANNELS = 32


def draw_antenna_pairs(key, part):
    first_list, second_list = jnp.triu_indices(S, 1)
    key_permute, key_reverse = jax.random.split(jax.random.fold_in(key, 11))
    sorted_index = jax.random.permutation(key_permute, STATION_PAIRS)
    reversed_pairs = jax.random.randint(key_reverse, (STATION_PAIRS,), 0, 2)
    first_list = first_list[sorted_index]
    second_list = second_list[sorted_index]
    lower = jnp.where(reversed_pairs == 1, second_list, first_list)
    upper = jnp.where(reversed_pairs == 1, first_list, second_list)
    return jnp.stack([lower, upper]).astype(jnp.int32)


def block_levels(own_key, shape, cuts, low, top_value):
    factor_of, own = 1.0, jax.random.fold_in(own_key, 6)
    for dim, shards_of in cuts:
        draws = jnp.exp(jax.random.uniform(jax.random.fold_in(own, dim), (shards_of,), jnp.float32, low / len(cuts), top_value / len(cuts)))
        factor_of = factor_of * jnp.repeat(draws, shape[dim] // shards_of).reshape([-1 if axis == dim else 1 for axis in range(len(shape))])
    return factor_of


def gaussian(key, dims, width, reach, shards=(), held_as=jnp.bfloat16):
    array = width * jax.random.normal(key, dims, jnp.float32)
    if shards:
        array = array * block_levels(key, dims, shards, -0.22, 0.18)
    return jnp.clip(array, -reach, reach).astype(held_as)


def setup_inputs(seed: int = 0) -> dict:
    key_list = jax.random.split(jax.random.key(seed), 13)
    measured_real = gaussian(key_list[0], (TIME_SLOTS, FREQ_CHANNELS, STATION_PAIRS), 10.0, 60.0, ((0, 8), (1, 32)), jnp.float32)
    measured_imaginary = gaussian(key_list[1], (TIME_SLOTS, FREQ_CHANNELS, STATION_PAIRS), 10.0, 60.0, ((0, 8), (1, 32)), jnp.float32)
    measured_weight = jnp.clip(jnp.exp(math.log(3.0) - 2.3025851 * jax.random.uniform(key_list[2], (TIME_SLOTS, FREQ_CHANNELS, STATION_PAIRS), jnp.float32) ** block_levels(key_list[2], (TIME_SLOTS, FREQ_CHANNELS, STATION_PAIRS), ((0, 8), (1, 32)), -0.2, 0.2)), 0.3, 3.0)
    baseline_vectors = gaussian(key_list[3], (TIME_SLOTS, 3, STATION_PAIRS), 20.0, 120.0, ((0, 8),), jnp.float32)
    antenna_pairs = draw_antenna_pairs(jax.random.fold_in(key_list[12], 71), 0)
    directions = gaussian(key_list[5], (3, D), 0.02, 0.12, (), jnp.float32)
    direction_flux = jnp.clip(jnp.exp(math.log(2.0) - 2.3025851 * jax.random.uniform(key_list[6], (FREQ_CHANNELS, D), jnp.float32) ** block_levels(key_list[6], (FREQ_CHANNELS, D), ((0, 32),), -0.2, 0.2)), 0.2, 2.0)
    channel_frequency = jnp.clip(1.1 + 0.79999995 * jax.random.uniform(key_list[7], (FREQ_CHANNELS,), jnp.float32) ** block_levels(key_list[7], (FREQ_CHANNELS,), ((0, 32),), -0.2, 0.2), 1.1, 1.9)
    electron_content_start = gaussian(key_list[8], (TIME_SLOTS, S, D), 1.0, 6.0, ((0, 8),), jnp.float32)
    pierce_station_direction = jax.vmap(lambda own: jax.random.permutation(own, P_SIZE))(jax.random.split(key_list[9], TIME_SLOTS)).reshape((TIME_SLOTS, P_SIZE)).astype(jnp.int32)
    eigen_basis = gaussian(key_list[10], (P_SIZE, K), P_SIZE ** -0.5, 0.0546875, ((0, 32),), jnp.float32)
    eigen_weight = jnp.clip(jnp.exp(jax.random.uniform(key_list[11], (K,), jnp.float32, math.log(0.1), math.log(1.0))), 0.1, 1.0)
    return dict(measured_real=measured_real, measured_imaginary=measured_imaginary, measured_weight=measured_weight, baseline_vectors=baseline_vectors, antenna_pairs=antenna_pairs, directions=directions, direction_flux=direction_flux, channel_frequency=channel_frequency, electron_content_start=electron_content_start, pierce_station_direction=pierce_station_direction, eigen_basis=eigen_basis, eigen_weight=eigen_weight)


HIGHEST = lax.Precision.HIGHEST
TEC_PHASE = -0.8448
SMOOTHING = 0.5
TWO_PI = 6.283185307179586


def station_polarity(antenna_pairs):
    station_list = jnp.arange(S, dtype=jnp.int32)[:, None]
    first_match = (antenna_pairs[0][None, :] == station_list).astype(jnp.float32)
    second_match = (antenna_pairs[1][None, :] == station_list).astype(jnp.float32)
    return first_match - second_match, first_match + second_match


def pair_terms(vis_real, vis_imag, weights, coords, frequency, fluxes, tec_slot, signed_terms, directions):
    geometry = (TWO_PI * frequency) * jnp.dot(coords.T, directions, precision=HIGHEST)
    station_phase = (TEC_PHASE / frequency) * tec_slot
    phases = geometry + jnp.dot(signed_terms.T, station_phase, precision=HIGHEST)
    model_real = fluxes[None, :] * jnp.cos(phases)
    model_imag = fluxes[None, :] * jnp.sin(phases)
    leftover_real = vis_real - jnp.sum(model_real, axis=1)
    leftover_imaginary = vis_imag - jnp.sum(model_imag, axis=1)
    projected = weights[:, None] * (model_real * leftover_imaginary[:, None] - model_imag * leftover_real[:, None])
    numerator = (TEC_PHASE / frequency) * jnp.dot(signed_terms, projected, precision=HIGHEST)
    return numerator, leftover_real, leftover_imaginary


def reference(measured_real, measured_imaginary, measured_weight, baseline_vectors, antenna_pairs, directions, direction_flux, channel_frequency, electron_content_start, pierce_station_direction, eigen_basis, eigen_weight):
    signed_terms, station_touches = station_polarity(antenna_pairs)
    tec_scale = TEC_PHASE / channel_frequency
    station_weight = jnp.einsum('sb,tfb->tfs', station_touches, measured_weight, precision=HIGHEST)
    denominator = jnp.einsum('tfs,fd->tsd', station_weight * (tec_scale * tec_scale)[None, :, None], direction_flux * direction_flux, precision=HIGHEST)
    slot_count = electron_content_start.shape[0]
    denom_flat = denominator.reshape(slot_count, -1)
    tec_flat = electron_content_start.reshape(slot_count, -1)
    slot_rows = jnp.arange(slot_count, dtype=jnp.int32)[:, None]
    position = jnp.arange(slot_count, dtype=jnp.int32)
    neighbours = (position > 0).astype(jnp.float32) + (position < slot_count - 1).astype(jnp.float32)
    smooth = None
    leftover_real = None
    leftover_imaginary = None
    for iteration in range(ITERS):
        current = tec_flat

        def slot_terms(slot_index):
            tec_slot = current[slot_index].reshape(S, D)

            def channel_step(running, channel):
                numerator, part_real, part_imag = pair_terms(measured_real[slot_index, channel], measured_imaginary[slot_index, channel], measured_weight[slot_index, channel], baseline_vectors[slot_index], channel_frequency[channel], direction_flux[channel], tec_slot, signed_terms, directions)
                return running + numerator, (part_real, part_imag)

            running, (part_real, part_imag) = lax.scan(channel_step, jnp.zeros((S, D), jnp.float32), jnp.arange(FREQ_CHANNELS, dtype=jnp.int32))
            return running, part_real, part_imag

        numerator, leftover_real, leftover_imaginary = lax.map(slot_terms, jnp.arange(slot_count, dtype=jnp.int32))
        update = current + numerator.reshape(slot_count, -1) / denom_flat
        target = jnp.take_along_axis(update, pierce_station_direction, axis=1)
        raw = eigen_weight[None, :] * jnp.dot(target, eigen_basis, precision=HIGHEST)
        padded = jnp.pad(raw, ((1, 1), (0, 0)))
        smooth = (raw + SMOOTHING * (padded[:-2] + padded[2:])) / (1.0 + SMOOTHING * neighbours)[:, None]
        screen = jnp.dot(smooth, eigen_basis.T, precision=HIGHEST)
        tec_flat = jnp.zeros_like(screen).at[slot_rows, pierce_station_direction].set(screen)
    return tec_flat.reshape(slot_count, S, D), smooth, leftover_real, leftover_imaginary
```

```python
import jax
import jax.numpy as jnp
from jax import lax
from jax.experimental import pallas as pl
from jax.experimental.pallas import tpu as pltpu
from jax.sharding import PartitionSpec as P

ITERS = 4
TEC_PHASE = -0.8448
SMOOTHING = 0.5
TWO_PI = 6.283185307179586
INTERPRET = False

S, D, K, B = 60, 200, 2048, 1770
SP, DP, BP = 64, 208, 1792
CH, PB, PW = 32, 375, 384
LB = 256
F32, BF16 = jnp.float32, jnp.bfloat16

COS = (0.9999999891722796, -19.73920453209451, 64.93911898389003, -85.45016555018871,
       60.167831730030905, -25.968313296519984, 6.5296104072911)
SIN = (6.283185272722459, -41.341697068957856, 81.60502462263176, -76.70155117699308,
       42.016165826534845, -14.868611009881327, 3.199693676305946)


def horner(coefficients, z):
    value = coefficients[-1] * z + coefficients[-2]
    for term in coefficients[-3::-1]:
        value = value * z + term
    return value


def split3(x):
    high = x.astype(BF16).astype(F32)
    rest = x - high
    middle = rest.astype(BF16).astype(F32)
    return high, middle, rest - middle


def dot_nt(a, b):
    return lax.dot_general(a, b, (((1,), (1,)), ((), ())), preferred_element_type=F32)


def dot_nn(a, b):
    return lax.dot_general(a, b, (((1,), (0,)), ((), ())), preferred_element_type=F32)


def one_hot(numbers, rows):
    return lax.broadcasted_iota(jnp.int32, (rows, numbers.shape[1]), 0) == numbers


def placed_parts(vals, stations, dirs, i):
    v = jnp.concatenate([vals[2 * i], vals[2 * i + 1]], axis=1)
    s = jnp.concatenate([stations[2 * i], stations[2 * i + 1]], axis=1)
    d = jnp.concatenate([dirs[2 * i], dirs[2 * i + 1]], axis=1)
    at = one_hot(s, SP)
    by_station = jnp.concatenate(
        [jnp.where(at, part, 0.0).astype(BF16) for part in split3(v)], axis=0
    )
    by_direction = jnp.where(one_hot(d, DP), 1.0, 0.0).astype(BF16)
    return by_station, by_direction


def picked(parts, s, d):
    at = jnp.where(one_hot(s, SP), 1.0, 0.0).astype(BF16)
    rows = dot_nn(parts, jnp.concatenate([at, at, at], axis=0))
    return jnp.sum(jnp.where(one_hot(d, DP), rows, 0.0), axis=0, keepdims=True)


def stacked(field):
    return jnp.concatenate([part.astype(BF16) for part in split3(field)], axis=1)


def solver(scal, tec, vis, uvw, pairs, cols, stations, dirs, own, out, res, acc, re_s, im_s, first, own_out):
    turn_scale = scal[0]
    tec_scale = scal[1]
    if first:
        parts = stacked(tec[...])
        own_out[...] = picked(parts, own[0], own[1])
    else:
        acc[...] = jnp.zeros_like(acc)

        def place(i, carry):
            by_station, by_direction = placed_parts(tec, stations, dirs, i)
            acc[...] += dot_nt(by_direction, by_station)
            return carry

        lax.fori_loop(0, CH // 2, place, 0)
        parts = acc[...].astype(BF16)

    def chunk(j, carry):
        numer, weight_sum = carry
        lanes = pl.ds(pl.multiple_of(j * LB, LB), LB)
        first_at = one_hot(pairs[0:1, lanes], SP)
        second_at = one_hot(pairs[1:2, lanes], SP)
        sign = jnp.where(first_at, 1.0, jnp.where(second_at, -1.0, 0.0)).astype(BF16)
        mixed = dot_nn(parts, jnp.concatenate([sign, sign, sign], axis=0))
        coords = uvw[:, lanes]
        data = vis[:, lanes]
        sums = []
        for h in range(LB // 128):
            c = coords[:, h * 128 : (h + 1) * 128]
            sum_re = jnp.zeros((8, 128), F32)
            sum_im = jnp.zeros((8, 128), F32)
            for g in range(DP // 8):
                rows = slice(8 * g, 8 * g + 8)
                turns = (
                    cols[0, rows, :] * c[0:1, :]
                    + cols[1, rows, :] * c[1:2, :]
                    + cols[2, rows, :] * c[2:3, :]
                ) + turn_scale * mixed[rows, h * 128 : (h + 1) * 128]
                r = turns - jnp.round(turns)
                z = r * r
                flux = cols[3, rows, :]
                re = flux * horner(COS, z)
                im = flux * (r * horner(SIN, z))
                re_s[rows, h * 128 : (h + 1) * 128] = re
                im_s[rows, h * 128 : (h + 1) * 128] = im
                sum_re = sum_re + re
                sum_im = sum_im + im
            sums.append(
                (jnp.sum(sum_re, axis=0, keepdims=True), jnp.sum(sum_im, axis=0, keepdims=True))
            )
        left_re = data[0:1, :] - jnp.concatenate([a for a, _ in sums], axis=1)
        left_im = data[1:2, :] - jnp.concatenate([b for _, b in sums], axis=1)
        res[0:1, lanes] = left_re
        res[1:2, lanes] = left_im
        weight = data[2:3, :]
        proj = re_s[...] * (weight * left_im) - im_s[...] * (weight * left_re)
        high = proj.astype(BF16)
        low = (proj - high.astype(F32)).astype(BF16)
        numer = numer + (dot_nt(high, sign) + dot_nt(low, sign))
        if first:
            touched = jnp.where(first_at | second_at, weight, 0.0)
            weight_sum = weight_sum + (touched[:, :128] + touched[:, 128:])
        return numer, weight_sum

    numer, weight_sum = lax.fori_loop(
        0, BP // LB, chunk, (jnp.zeros((DP, SP), F32), jnp.zeros((SP, 128), F32))
    )
    numer_parts = stacked(numer * tec_scale)
    if first:
        weight_at = jnp.sum(weight_sum, axis=1, keepdims=True) * (tec_scale * tec_scale)
        flux_col = cols[3, :, 0:1]
        flux_col = flux_col * flux_col

    def pick(i, carry):
        s = jnp.concatenate([stations[2 * i], stations[2 * i + 1]], axis=1)
        d = jnp.concatenate([dirs[2 * i], dirs[2 * i + 1]], axis=1)
        got = picked(numer_parts, s, d)
        out[2 * i, 0:1, 0:PW] = got[:, :PW]
        out[2 * i + 1, 0:1, 0:PW] = got[:, PW:]
        if first:
            w_at = jnp.sum(jnp.where(one_hot(s, SP), weight_at, 0.0), axis=0, keepdims=True)
            f_at = jnp.sum(jnp.where(one_hot(d, DP), flux_col, 0.0), axis=0, keepdims=True)
            den = w_at * f_at
            out[2 * i, 0:1, PW : 2 * PW] = den[:, :PW]
            out[2 * i + 1, 0:1, PW : 2 * PW] = den[:, PW:]
        return carry

    lax.fori_loop(0, CH // 2, pick, 0)


def params():
    return dict(
        compiler_params=pltpu.CompilerParams(),
        interpret=pltpu.InterpretParams() if INTERPRET else False,
    )


VM = pl.BlockSpec(memory_space=pltpu.VMEM)
SM = pl.BlockSpec(memory_space=pltpu.SMEM)
HB = pl.BlockSpec(memory_space=pl.ANY)


def call(kernel, name, out_shape, in_specs, scratch=()):
    return pl.pallas_call(
        kernel,
        name=name,
        out_shape=[jax.ShapeDtypeStruct(s, F32) for s in out_shape],
        in_specs=in_specs,
        out_specs=[VM] * len(out_shape),
        scratch_shapes=list(scratch),
        **params(),
    )


def first_solver(scal, tec, vis, uvw, pairs, cols, stations, dirs, own):
    def kernel(scal, tec, vis, uvw, pairs, cols, stations, dirs, own, out, res, own_out, re_s, im_s):
        solver(scal, tec, vis, uvw, pairs, cols, stations, dirs, own, out, res, None, re_s, im_s, True, own_out)

    return call(
        kernel,
        "first_solver",
        [(CH, 1, 2 * PW), (2, BP), (1, PW)],
        [SM] + [VM] * 8,
        [pltpu.VMEM((DP, LB), F32), pltpu.VMEM((DP, LB), F32)],
    )(scal, tec, vis, uvw, pairs, cols, stations, dirs, own)


def next_solver(scal, tec, vis, uvw, pairs, cols, stations, dirs):
    def kernel(scal, tec, vis, uvw, pairs, cols, stations, dirs, out, res, acc, re_s, im_s):
        solver(scal, tec, vis, uvw, pairs, cols, stations, dirs, None, out, res, acc, re_s, im_s, False, None)

    return call(
        kernel,
        "next_solver",
        [(CH, 1, PW), (2, BP)],
        [SM] + [VM] * 7,
        [pltpu.VMEM((DP, 3 * SP), F32), pltpu.VMEM((DP, LB), F32), pltpu.VMEM((DP, LB), F32)],
    )(scal, tec, vis, uvw, pairs, cols, stations, dirs)


def final_place(vals, stations, dirs):
    def kernel(vals, stations, dirs, out, acc):
        acc[...] = jnp.zeros_like(acc)

        def place(i, carry):
            by_station, by_direction = placed_parts(vals, stations, dirs, i)
            acc[...] += dot_nt(by_station, by_direction)
            return carry

        lax.fori_loop(0, CH // 2, place, 0)
        out[...] = (acc[0:SP, :] + acc[SP : 2 * SP, :]) + acc[2 * SP : 3 * SP, :]

    return call(kernel, "final_place", [(SP, DP)], [VM] * 3, [pltpu.VMEM((3 * SP, DP), F32)])(
        vals, stations, dirs
    )[0]


def own_target(arrived, own, denominator):
    first = denominator is None

    def kernel(arrived, own, *refs):
        total = jnp.sum(arrived[...], axis=0)
        if first:
            out, den_out = refs
            den = total[:, PW:]
            den_out[...] = den
        else:
            den_ref, out = refs
            den = den_ref[...]
        lane = lax.broadcasted_iota(jnp.int32, (1, PW), 1)
        out[...] = jnp.where(lane < PB, own[...] + total[:, :PW] / den, 0.0)

    if first:
        return call(kernel, "own_target_first", [(1, PW), (1, PW)], [VM] * 2)(arrived, own)
    return call(kernel, "own_target", [(1, PW)], [VM] * 3)(arrived, own, denominator)[0], denominator


CUTS = ((0, 96), (96, 96), (192, 96), (288, 87))


def basis_copies(basis, held, sems):
    copies = [
        pltpu.make_async_copy(basis.at[pl.ds(a, n)], held.at[pl.ds(a, n)], sems.at[i])
        for i, (a, n) in enumerate(CUTS)
    ]
    for copy in copies:
        copy.start()
    return copies


def groups_of(a, n):
    return [(r, min(8, a + n - r)) for r in range(a, a + n, 8)]


BASIS_SCRATCH = [pltpu.VMEM((PB, K), F32), pltpu.SemaphoreType.DMA((len(CUTS),))]


def basis_partial(norm, target, near, far, weight, basis):
    def kernel(norm, target, near, far, weight, basis, out, held, sems, tall):
        copies = basis_copies(basis, held, sems)
        x = (target[...] + SMOOTHING * (near[...] + far[...])) / norm[0]
        tall[...] = jnp.broadcast_to(x, (128, PW)).T
        total = jnp.zeros((8, K), F32)
        tail = jnp.zeros((1, K), F32)
        for copy, (a, n) in zip(copies, CUTS):
            copy.wait()
            for r, m in groups_of(a, n):
                column = tall[r : r + m, :]
                piece = held[r : r + m, :] * jnp.concatenate([column] * (K // 128), axis=1)
                if m == 8:
                    total = total + piece
                else:
                    tail = jnp.sum(piece, axis=0, keepdims=True)
        row = (jnp.sum(total, axis=0, keepdims=True) + tail) * weight[...]
        for c in range(CH):
            out[c] = row

    return call(
        kernel,
        "basis_partial",
        [(CH, 1, K)],
        [SM] + [VM] * 4 + [HB],
        BASIS_SCRATCH + [pltpu.VMEM((PW, 128), F32)],
    )(norm, target, near, far, weight, basis)[0]


def own_screen(arrived, basis):
    def kernel(arrived, basis, coef, own, out, held, sems, tall):
        copies = basis_copies(basis, held, sems)
        row = jnp.sum(arrived[...], axis=0)
        coef[...] = row
        spread = jnp.broadcast_to(row, (8, K))
        tall[PW - 16 : PW, :] = jnp.zeros((16, 128), F32)
        for copy, (a, n) in zip(copies, CUTS):
            copy.wait()
            for r, m in groups_of(a, n):
                piece = held[r : r + m, :] * spread[0:m, :]
                parts = [piece[:, k : k + 128] for k in range(0, K, 128)]
                while len(parts) > 1:
                    parts = [u + v for u, v in zip(parts[0::2], parts[1::2])]
                tall[r : r + m, :] = parts[0]
        line = jnp.sum(tall[...].T, axis=0, keepdims=True)
        own[...] = line
        for c in range(CH):
            out[c] = line

    return call(
        kernel,
        "own_screen",
        [(1, K), (1, PW), (CH, 1, PW)],
        [VM, HB],
        BASIS_SCRATCH + [pltpu.VMEM((PW, 128), F32)],
    )(arrived, basis)


def exchange(value):
    return lax.all_to_all(value, "chan", split_axis=0, concat_axis=0, tiled=True)


def per_device(
    measured_real,
    measured_imaginary,
    measured_weight,
    baseline_vectors,
    antenna_pairs,
    directions,
    direction_flux,
    channel_frequency,
    electron_content_start,
    pierce_station_direction,
    eigen_basis,
    eigen_weight,
):
    frequency = channel_frequency[0]
    tec_scale = TEC_PHASE / frequency
    scal = jnp.stack([tec_scale * (1.0 / TWO_PI), tec_scale])
    vis = jnp.concatenate(
        [measured_real[0], measured_imaginary[0], measured_weight[0]], axis=0
    )
    vis = jnp.pad(vis, ((0, 0), (0, BP - B)))
    uvw = jnp.pad(baseline_vectors[0] * frequency, ((0, 0), (0, BP - B)))
    pairs = jnp.pad(antenna_pairs, ((0, 0), (0, BP - B)), constant_values=-1)
    cols = jnp.concatenate([directions, direction_flux], axis=0)
    cols = jnp.broadcast_to(jnp.pad(cols, ((0, 0), (0, DP - D)))[:, :, None], (4, DP, 128))
    tec_start = jnp.pad(electron_content_start[0].T, ((0, DP - D), (0, SP - S)))
    points = pierce_station_direction[0].reshape(CH, 1, PB)
    fill = ((0, 0), (0, 0), (0, PW - PB))
    stations = jnp.pad(points // D, fill, constant_values=-1)
    dirs = jnp.pad(points % D, fill, constant_values=-1)
    mine = lax.axis_index("chan")
    own_points = jnp.stack(
        [
            lax.dynamic_index_in_dim(stations, mine, 0, keepdims=False),
            lax.dynamic_index_in_dim(dirs, mine, 0, keepdims=False),
        ]
    )
    slot = lax.axis_index("slot")
    slots = lax.axis_size("slot")
    inside = (slot > 0).astype(F32) + (slot < slots - 1).astype(F32)
    norm = (1.0 + SMOOTHING * inside).reshape(1)
    weight = eigen_weight[None, :]
    near_pairs = [(i, i ^ 1) for i in range(slots) if i ^ 1 < slots]
    far_pairs = [(i, i - 1 if i % 2 == 0 else i + 1) for i in range(1, slots - 1)]
    far_pairs = [(i, j) for i, j in far_pairs if 0 <= j < slots]
    own = None
    denominator = None
    gathered = None
    coefficients = None
    residual = None
    for iteration in range(ITERS):
        if iteration == 0:
            sent, residual, own = first_solver(
                scal, tec_start, vis, uvw, pairs, cols, stations, dirs, own_points
            )
        else:
            sent, residual = next_solver(
                scal, gathered, vis, uvw, pairs, cols, stations, dirs
            )
        target, denominator = own_target(exchange(sent), own, denominator)
        far = lax.ppermute(target, "slot", far_pairs)
        near = lax.ppermute(target, "slot", near_pairs)
        partial = basis_partial(norm, target, near, far, weight, eigen_basis)
        coefficients, own, spread = own_screen(exchange(partial), eigen_basis)
        gathered = exchange(spread)
    tec_final = final_place(gathered, stations, dirs)[:S, :D]
    return (
        tec_final[None],
        coefficients,
        residual[0:1, :B][None],
        residual[1:2, :B][None],
    )


def solution(mesh):
    in_specs = (
        P("slot", "chan", None),
        P("slot", "chan", None),
        P("slot", "chan", None),
        P("slot", None, None),
        P(),
        P(),
        P("chan", None),
        P("chan"),
        P("slot", None, None),
        P("slot", None),
        P("chan", None),
        P(),
    )
    out_specs = (
        P("slot", None, None),
        P("slot", None),
        P("slot", "chan", None),
        P("slot", "chan", None),
    )
    return jax.shard_map(
        per_device, mesh=mesh, in_specs=in_specs, out_specs=out_specs, check_vma=False
    )
```

```python
import jax
import jax.numpy as jnp
from jax import lax
from jax.experimental import pallas as pl
from jax.experimental.pallas import tpu as pltpu
from jax.sharding import PartitionSpec as P

ITERS = 4
TEC_PHASE = -0.8448
SMOOTHING = 0.5
TWO_PI = 6.283185307179586
INTERPRET = False
VMEM_LIMIT = 16 * 1024 * 1024

S, D, K, B = 60, 200, 2048, 1770
SP, DP, BP = 64, 208, 1792
CH, PB, PW = 32, 375, 384
LB = 256
F32, BF16 = jnp.float32, jnp.bfloat16

COS = (0.9999999891722796, -19.73920453209451, 64.93911898389003, -85.45016555018871,
       60.167831730030905, -25.968313296519984, 6.5296104072911)
SIN = (6.283185272722459, -41.341697068957856, 81.60502462263176, -76.70155117699308,
       42.016165826534845, -14.868611009881327, 3.199693676305946)


def horner(coefficients, z):
    value = coefficients[-1] * z + coefficients[-2]
    for term in coefficients[-3::-1]:
        value = value * z + term
    return value


def split3(x):
    high = x.astype(BF16).astype(F32)
    rest = x - high
    middle = rest.astype(BF16).astype(F32)
    return high, middle, rest - middle


def dot_nt(a, b):
    return lax.dot_general(a, b, (((1,), (1,)), ((), ())), preferred_element_type=F32)


def dot_nn(a, b):
    return lax.dot_general(a, b, (((1,), (0,)), ((), ())), preferred_element_type=F32)


def one_hot(numbers, rows):
    return lax.broadcasted_iota(jnp.int32, (rows, numbers.shape[1]), 0) == numbers


def placed_parts(vals, stations, dirs, i):
    v = jnp.concatenate([vals[2 * i], vals[2 * i + 1]], axis=1)
    s = jnp.concatenate([stations[2 * i], stations[2 * i + 1]], axis=1)
    d = jnp.concatenate([dirs[2 * i], dirs[2 * i + 1]], axis=1)
    at = one_hot(s, SP)
    by_station = jnp.concatenate(
        [jnp.where(at, part, 0.0).astype(BF16) for part in split3(v)], axis=0
    )
    by_direction = jnp.where(one_hot(d, DP), 1.0, 0.0).astype(BF16)
    return by_station, by_direction


def picked(parts, s, d):
    at = jnp.where(one_hot(s, SP), 1.0, 0.0).astype(BF16)
    rows = dot_nn(parts, jnp.concatenate([at, at, at], axis=0))
    return jnp.sum(jnp.where(one_hot(d, DP), rows, 0.0), axis=0, keepdims=True)


def stacked(field):
    return jnp.concatenate([part.astype(BF16) for part in split3(field)], axis=1)


def solver(freq, tec, vis, uvw, pairs, cols, stations, dirs, out, work, own=None, kept=None):
    acc, re_s, im_s = work
    tec_scale = TEC_PHASE / freq[...]
    turn_scale = jnp.broadcast_to(tec_scale * (1.0 / TWO_PI), (8, 128))
    first = own is not None
    if first:
        parts, mine, own_out = own
        own_out[...] = picked(parts, stations[mine], dirs[mine])
    else:
        acc[...] = jnp.zeros_like(acc)

        def place(i, carry):
            by_station, by_direction = placed_parts(tec, stations, dirs, i)
            acc[...] += dot_nt(by_direction, by_station)
            return carry

        lax.fori_loop(0, CH // 2, place, 0)
        parts = acc[...].astype(BF16)

    def chunk(j, carry):
        numer, weight_sum = carry
        lanes = pl.ds(pl.multiple_of(j * LB, LB), LB)
        first_at = one_hot(pairs[0:1, lanes], SP)
        second_at = one_hot(pairs[1:2, lanes], SP)
        sign = jnp.where(first_at, 1.0, jnp.where(second_at, -1.0, 0.0)).astype(BF16)
        mixed = dot_nn(parts, jnp.concatenate([sign, sign, sign], axis=0))
        coords = uvw[:, lanes]
        data = vis[:, lanes]
        sums = []
        for h in range(LB // 128):
            c = coords[:, h * 128 : (h + 1) * 128]
            sum_re = jnp.zeros((8, 128), F32)
            sum_im = jnp.zeros((8, 128), F32)
            for g in range(DP // 8):
                rows = slice(8 * g, 8 * g + 8)
                turns = (
                    cols[0, rows, :] * c[0:1, :]
                    + cols[1, rows, :] * c[1:2, :]
                    + cols[2, rows, :] * c[2:3, :]
                ) + turn_scale * mixed[rows, h * 128 : (h + 1) * 128]
                r = turns - jnp.round(turns)
                z = r * r
                flux = cols[3, rows, :]
                re = flux * horner(COS, z)
                im = flux * (r * horner(SIN, z))
                re_s[rows, h * 128 : (h + 1) * 128] = re
                im_s[rows, h * 128 : (h + 1) * 128] = im
                sum_re = sum_re + re
                sum_im = sum_im + im
            sums.append(
                (jnp.sum(sum_re, axis=0, keepdims=True), jnp.sum(sum_im, axis=0, keepdims=True))
            )
        left_re = data[0:1, :] - jnp.concatenate([a for a, _ in sums], axis=1)
        left_im = data[1:2, :] - jnp.concatenate([b for _, b in sums], axis=1)
        if kept is not None:
            kept[0][0:1, lanes] = left_re
            kept[0][1:2, lanes] = left_im
        weight = data[2:3, :]
        proj = re_s[...] * (weight * left_im) - im_s[...] * (weight * left_re)
        high = proj.astype(BF16)
        low = (proj - high.astype(F32)).astype(BF16)
        numer = numer + (dot_nt(high, sign) + dot_nt(low, sign))
        if first:
            touched = jnp.where(first_at | second_at, weight, 0.0)
            weight_sum = weight_sum + (touched[:, :128] + touched[:, 128:])
        return numer, weight_sum

    numer, weight_sum = lax.fori_loop(
        0, BP // LB, chunk, (jnp.zeros((DP, SP), F32), jnp.zeros((SP, 128), F32))
    )
    if kept is not None:
        kept[1][0] = kept[0][0:1, 0:B]
        kept[2][0] = kept[0][1:2, 0:B]
    numer_parts = stacked(numer * tec_scale)
    if first:
        weight_at = jnp.sum(weight_sum, axis=1, keepdims=True) * (tec_scale * tec_scale)
        flux_col = cols[3, :, 0:1]
        flux_col = flux_col * flux_col

    def pick(i, carry):
        s = jnp.concatenate([stations[2 * i], stations[2 * i + 1]], axis=1)
        d = jnp.concatenate([dirs[2 * i], dirs[2 * i + 1]], axis=1)
        got = picked(numer_parts, s, d)
        out[2 * i, 0:1, 0:PW] = got[:, :PW]
        out[2 * i + 1, 0:1, 0:PW] = got[:, PW:]
        if first:
            w_at = jnp.sum(jnp.where(one_hot(s, SP), weight_at, 0.0), axis=0, keepdims=True)
            f_at = jnp.sum(jnp.where(one_hot(d, DP), flux_col, 0.0), axis=0, keepdims=True)
            den = w_at * f_at
            out[2 * i, 0:1, PW : 2 * PW] = den[:, :PW]
            out[2 * i + 1, 0:1, PW : 2 * PW] = den[:, PW:]
        return carry

    lax.fori_loop(0, CH // 2, pick, 0)


def params():
    return dict(
        compiler_params=pltpu.CompilerParams(vmem_limit_bytes=VMEM_LIMIT),
        interpret=pltpu.InterpretParams() if INTERPRET else False,
    )


VM = pl.BlockSpec(memory_space=pltpu.VMEM)
SM = pl.BlockSpec(memory_space=pltpu.SMEM)


def call(kernel, name, out_shape, in_specs, scratch=()):
    return pl.pallas_call(
        kernel,
        name=name,
        out_shape=[
            s if isinstance(s, jax.ShapeDtypeStruct) else jax.ShapeDtypeStruct(s, F32)
            for s in out_shape
        ],
        in_specs=in_specs,
        out_specs=[VM] * len(out_shape),
        scratch_shapes=list(scratch),
        **params(),
    )


WORK = [
    pltpu.VMEM((DP, 3 * SP), F32),
    pltpu.VMEM((DP, LB), F32),
    pltpu.VMEM((DP, LB), F32),
]


def first_solver(ids, freq, real, imag, weight, coords, pairs, directions, flux, start, points):
    def kernel(
        ids, freq, real, imag, weight, coords, pairs, directions, flux, start, points,
        out, own, vis, uvw, ants, cols, stations, dirs, acc, re_s, im_s, rows, tall,
    ):
        vis[...] = jnp.zeros_like(vis)
        vis[0:1, 0:B] = real[0]
        vis[1:2, 0:B] = imag[0]
        vis[2:3, 0:B] = weight[0]
        uvw[...] = jnp.zeros_like(uvw)
        uvw[:, 0:B] = coords[0] * freq[...]
        ants[...] = jnp.full(ants.shape, -1, jnp.int32)
        ants[:, 0:B] = pairs[...]
        rows[...] = jnp.zeros_like(rows)
        rows[0:3, 0:D] = directions[...]
        rows[3:4, 0:D] = flux[...]
        for c in range(4):
            cols[c] = jnp.broadcast_to(rows[c : c + 1, :], (128, 256)).T[:DP, :]
        tall[...] = jnp.zeros_like(tall)
        tall[0:S, 0:D] = start[0]
        parts = stacked(tall[...].T[:DP, :SP])
        q = points[...]
        s = jnp.floor((q.astype(F32) + 0.5) * (1.0 / D)).astype(jnp.int32)
        d = q - s * D
        blank = jnp.full((1, PW), -1, jnp.int32)
        for c in range(CH):
            stations[c] = blank
            stations[c, 0:1, 0:PB] = s[:, c * PB : (c + 1) * PB]
            dirs[c] = blank
            dirs[c, 0:1, 0:PB] = d[:, c * PB : (c + 1) * PB]
        solver(
            freq, None, vis, uvw, ants, cols, stations, dirs, out, (acc, re_s, im_s),
            own=(parts, ids[0], own),
        )

    i32 = lambda *shape: jax.ShapeDtypeStruct(shape, jnp.int32)
    return call(
        kernel,
        "first_solver",
        [
            (CH, 1, 2 * PW), (1, PW), (3, BP), (3, BP), i32(2, BP), (4, DP, 128),
            i32(CH, 1, PW), i32(CH, 1, PW),
        ],
        [SM] + [VM] * 10,
        WORK + [pltpu.VMEM((8, 256), F32), pltpu.VMEM((128, 256), F32)],
    )(ids, freq, real, imag, weight, coords, pairs, directions, flux, start, points)


def next_solver(freq, tec, held, last):
    def kernel(freq, tec, vis, uvw, ants, cols, stations, dirs, out, *refs):
        if last:
            real, imag, acc, re_s, im_s, left = refs
            kept = (left, real, imag)
        else:
            acc, re_s, im_s = refs
            kept = None
        solver(
            freq, tec, vis, uvw, ants, cols, stations, dirs, out, (acc, re_s, im_s), kept=kept
        )

    return call(
        kernel,
        "last_solver" if last else "next_solver",
        [(CH, 1, PW)] + ([(1, 1, B), (1, 1, B)] if last else []),
        [VM] * 8,
        WORK + ([pltpu.VMEM((2, BP), F32)] if last else []),
    )(freq, tec, *held)


def final_place(vals, stations, dirs):
    def kernel(vals, stations, dirs, out, acc):
        acc[...] = jnp.zeros_like(acc)

        def place(i, carry):
            by_station, by_direction = placed_parts(vals, stations, dirs, i)
            acc[...] += dot_nt(by_station, by_direction)
            return carry

        lax.fori_loop(0, CH // 2, place, 0)
        whole = (acc[0:SP, :] + acc[SP : 2 * SP, :]) + acc[2 * SP : 3 * SP, :]
        out[0] = whole[:S, :D]

    return call(kernel, "final_place", [(1, S, D)], [VM] * 3, [pltpu.VMEM((3 * SP, DP), F32)])(
        vals, stations, dirs
    )[0]


def own_target(arrived, own, denominator):
    first = denominator is None

    def kernel(arrived, own, *refs):
        total = jnp.sum(arrived[...], axis=0)
        if first:
            out, den_out = refs
            den = total[:, PW:]
            den_out[...] = den
        else:
            den_ref, out = refs
            den = den_ref[...]
        lane = lax.broadcasted_iota(jnp.int32, (1, PW), 1)
        out[...] = jnp.where(lane < PB, own[...] + total[:, :PW] / den, 0.0)

    if first:
        return call(kernel, "own_target_first", [(1, PW), (1, PW)], [VM] * 2)(arrived, own)
    return call(kernel, "own_target", [(1, PW)], [VM] * 3)(arrived, own, denominator)[0], denominator


GROUPS = [(r, min(8, PB - r)) for r in range(0, PB, 8)]


def basis_partial(ids, slots, target, near, far, weight, basis):
    def kernel(ids, target, near, far, weight, basis, out, tall):
        slot = ids[1]
        ends = (slot == 0).astype(F32) + (slot == slots - 1).astype(F32)
        x = (target[...] + SMOOTHING * (near[...] + far[...])) / (1.0 + SMOOTHING * (2.0 - ends))
        tall[...] = jnp.broadcast_to(x, (128, PW)).T
        total = jnp.zeros((8, K), F32)
        for r, m in GROUPS:
            piece = basis[r : r + m, :] * jnp.concatenate([tall[r : r + m, :]] * (K // 128), axis=1)
            if m == 8:
                total = total + piece
        row = jnp.sum(total, axis=0, keepdims=True) + jnp.sum(piece, axis=0, keepdims=True)
        row = row * weight[...]
        for c in range(CH):
            out[c] = row

    return call(
        kernel,
        "basis_partial",
        [(CH, 1, K)],
        [SM] + [VM] * 5,
        [pltpu.VMEM((PW, 128), F32)],
    )(ids, target, near, far, weight, basis)[0]


def own_screen(arrived, basis):
    def kernel(arrived, basis, coef, own, out, tall):
        row = jnp.sum(arrived[...], axis=0)
        coef[...] = row
        spread = jnp.broadcast_to(row, (8, K))
        tall[PW - 16 : PW, :] = jnp.zeros((16, 128), F32)
        for r, m in GROUPS:
            piece = basis[r : r + m, :] * spread[0:m, :]
            parts = [piece[:, k : k + 128] for k in range(0, K, 128)]
            while len(parts) > 1:
                parts = [u + v for u, v in zip(parts[0::2], parts[1::2])]
            tall[r : r + m, :] = parts[0]
        line = jnp.sum(tall[...].T, axis=0, keepdims=True)
        own[...] = line
        for c in range(CH):
            out[c] = line

    return call(
        kernel,
        "own_screen",
        [(1, K), (1, PW), (CH, 1, PW)],
        [VM, VM],
        [pltpu.VMEM((PW, 128), F32)],
    )(arrived, basis)


def exchange(value):
    return lax.all_to_all(value, "chan", split_axis=0, concat_axis=0, tiled=True)


def per_device(
    measured_real,
    measured_imaginary,
    measured_weight,
    baseline_vectors,
    antenna_pairs,
    directions,
    direction_flux,
    channel_frequency,
    electron_content_start,
    pierce_station_direction,
    eigen_basis,
    eigen_weight,
):
    slots = lax.axis_size("slot")
    ids = jnp.stack([lax.axis_index("chan"), lax.axis_index("slot")]).astype(jnp.int32)
    freq = channel_frequency.reshape(1, 1)
    weight = eigen_weight[None, :]
    near_pairs = [(i, i ^ 1) for i in range(slots) if i ^ 1 < slots]
    far_pairs = [(i, i - 1 if i % 2 == 0 else i + 1) for i in range(1, slots - 1)]
    far_pairs = [(i, j) for i, j in far_pairs if 0 <= j < slots]
    sent, own, *held = first_solver(
        ids, freq, measured_real, measured_imaginary, measured_weight, baseline_vectors,
        antenna_pairs, directions, direction_flux, electron_content_start, pierce_station_direction,
    )
    denominator = None
    for iteration in range(ITERS):
        if iteration > 0:
            sent, *left = next_solver(freq, gathered, held, iteration == ITERS - 1)
        target, denominator = own_target(exchange(sent), own, denominator)
        far = lax.ppermute(target, "slot", far_pairs)
        near = lax.ppermute(target, "slot", near_pairs)
        partial = basis_partial(ids, slots, target, near, far, weight, eigen_basis)
        coefficients, own, spread = own_screen(exchange(partial), eigen_basis)
        gathered = exchange(spread)
    tec_final = final_place(gathered, held[4], held[5])
    return tec_final, coefficients, left[0], left[1]


def solution(mesh):
    in_specs = (
        P("slot", "chan", None),
        P("slot", "chan", None),
        P("slot", "chan", None),
        P("slot", None, None),
        P(),
        P(),
        P("chan", None),
        P("chan"),
        P("slot", None, None),
        P("slot", None),
        P("chan", None),
        P(),
    )
    out_specs = (
        P("slot", None, None),
        P("slot", None),
        P("slot", "chan", None),
        P("slot", "chan", None),
    )
    return jax.shard_map(
        per_device, mesh=mesh, in_specs=in_specs, out_specs=out_specs, check_vma=False
    )
```

```python
import jax
import jax.numpy as jnp
from jax import lax
from jax.experimental import pallas as pl
from jax.experimental.pallas import tpu as pltpu
from jax.sharding import PartitionSpec as P

ITERS = 4
TEC_PHASE = -0.8448
SMOOTHING = 0.5
TWO_PI = 6.283185307179586
INTERPRET = False
VMEM_LIMIT = 16 * 1024 * 1024

S, D, K, B = 60, 200, 2048, 1770
SP, DP, BP = 64, 208, 1792
CH, PB, PW = 32, 375, 384
LB = 256
NB = 16
F32, BF16 = jnp.float32, jnp.bfloat16

COS = (1.4142134965650244, -6.978850988240614, 5.7394611707149, -1.883562987515013, 0.3106981922394431)
SIN = (4.4428828341499464, -7.308241154547178, 3.606288958237895, -0.8457635962132565, 0.10920575375700989)

PRODUCTS = ((0, 0), (0, 1), (1, 0), (1, 1), (0, 2), (2, 0))
GP = 32


def horner(coefficients, z):
    value = coefficients[-1] * z + coefficients[-2]
    for term in coefficients[-3::-1]:
        value = value * z + term
    return value


def split3(x):
    high = x.astype(BF16).astype(F32)
    rest = x - high
    middle = rest.astype(BF16).astype(F32)
    return high, middle, rest - middle


def dot_nt(a, b):
    return lax.dot_general(a, b, (((1,), (1,)), ((), ())), preferred_element_type=F32)


def dot_nn(a, b):
    return lax.dot_general(a, b, (((1,), (0,)), ((), ())), preferred_element_type=F32)


def one_hot(numbers, rows):
    return lax.broadcasted_iota(jnp.int32, (rows, numbers.shape[1]), 0) == numbers


def joined(blocks, i):
    return jnp.concatenate([blocks[NB * i + k] for k in range(NB)], axis=1)


def placed_parts(vals, stations, dirs, i):
    v, s, d = joined(vals, i), joined(stations, i), joined(dirs, i)
    at = one_hot(s, SP)
    by_station = jnp.concatenate(
        [jnp.where(at, part, 0.0).astype(BF16) for part in split3(v)], axis=0
    )
    by_direction = jnp.where(one_hot(d, DP), 1.0, 0.0).astype(BF16)
    return by_station, by_direction


def picked(parts, s, d):
    at = jnp.where(one_hot(s, SP), 1.0, 0.0).astype(BF16)
    rows = dot_nn(parts, jnp.concatenate([at, at, at], axis=0))
    return jnp.sum(jnp.where(one_hot(d, DP), rows, 0.0), axis=0, keepdims=True)


def stacked(field):
    return jnp.concatenate([part.astype(BF16) for part in split3(field)], axis=1)


def solver(freq, tec, vis, base, coords, pairs, cols, stations, dirs, out, work, own=None, kept=None):
    acc, re_s, im_s = work
    tec_scale = TEC_PHASE / freq[...]
    turn_scale = jnp.broadcast_to(tec_scale * (1.0 / TWO_PI), (8, 128))
    first = own is not None
    if first:
        tec_parts, base_parts, mine, own_out = own
        own_out[...] = picked(tec_parts, stations[mine], dirs[mine])
        parts = jnp.concatenate([tec_parts, base_parts], axis=1)
    else:
        acc[...] = base[...]

        def place(i, carry):
            by_station, by_direction = placed_parts(tec, stations, dirs, i)
            acc[:, 0 : 3 * SP] += dot_nt(by_direction, by_station)
            return carry

        lax.fori_loop(0, CH // NB, place, 0)
        parts = acc[...].astype(BF16)

    def chunk(j, carry):
        numer, weight_sum = carry
        lanes = pl.ds(j * LB, LB)
        first_at = one_hot(pairs[0:1, lanes], SP)
        second_at = one_hot(pairs[1:2, lanes], SP)
        sign = jnp.where(first_at, 1.0, jnp.where(second_at, -1.0, 0.0)).astype(BF16)
        mixed = dot_nn(
            parts, jnp.concatenate([sign, sign, sign, coords[:, lanes].astype(BF16)], axis=0)
        )
        data = vis[:, lanes]
        sums = []
        for h in range(LB // 128):
            sum_re = jnp.zeros((8, 128), F32)
            sum_im = jnp.zeros((8, 128), F32)
            for g in range(DP // 8):
                rows = slice(8 * g, 8 * g + 8)
                turns = turn_scale * mixed[rows, h * 128 : (h + 1) * 128]
                r = turns - jnp.round(turns)
                z = r * r
                flux = cols[rows, :]
                half_sin = r * horner(SIN, z)
                re = flux - flux * (half_sin * half_sin)
                im = flux * (half_sin * horner(COS, z))
                re_s[rows, h * 128 : (h + 1) * 128] = re
                im_s[rows, h * 128 : (h + 1) * 128] = im
                sum_re = sum_re + re
                sum_im = sum_im + im
            sums.append(
                (jnp.sum(sum_re, axis=0, keepdims=True), jnp.sum(sum_im, axis=0, keepdims=True))
            )
        left_re = data[0:1, :] - jnp.concatenate([a for a, _ in sums], axis=1)
        left_im = data[1:2, :] - jnp.concatenate([b for _, b in sums], axis=1)
        if kept is not None:
            kept[0][0:1, lanes] = left_re
            kept[0][1:2, lanes] = left_im
        weight = data[2:3, :]
        proj = re_s[...] * (weight * left_im) - im_s[...] * (weight * left_re)
        high = proj.astype(BF16)
        low = (proj - high.astype(F32)).astype(BF16)
        numer = numer + (dot_nt(high, sign) + dot_nt(low, sign))
        if first:
            touched = jnp.where(first_at | second_at, weight, 0.0)
            weight_sum = weight_sum + (touched[:, :128] + touched[:, 128:])
        return numer, weight_sum

    numer, weight_sum = jnp.zeros((DP, SP), F32), jnp.zeros((SP, 128), F32)
    for j in range(BP // LB):
        numer, weight_sum = chunk(j, (numer, weight_sum))
    if kept is not None:
        kept[1][0] = kept[0][0:1, 0:B]
        kept[2][0] = kept[0][1:2, 0:B]
    numer_parts = stacked(numer * tec_scale)
    if first:
        weight_at = jnp.sum(weight_sum, axis=1, keepdims=True) * (tec_scale * tec_scale)
        flux_col = cols[:, 0:1]
        flux_col = flux_col * flux_col

    def pick(i, carry):
        s, d = joined(stations, i), joined(dirs, i)
        got = picked(numer_parts, s, d)
        for k in range(NB):
            out[NB * i + k, 0:1, 0:PW] = got[:, k * PW : (k + 1) * PW]
        if first:
            w_at = jnp.sum(jnp.where(one_hot(s, SP), weight_at, 0.0), axis=0, keepdims=True)
            f_at = jnp.sum(jnp.where(one_hot(d, DP), flux_col, 0.0), axis=0, keepdims=True)
            den = w_at * f_at
            for k in range(NB):
                out[NB * i + k, 0:1, PW : 2 * PW] = den[:, k * PW : (k + 1) * PW]
        return carry

    lax.fori_loop(0, CH // NB, pick, 0)


def params():
    return dict(
        compiler_params=pltpu.CompilerParams(vmem_limit_bytes=VMEM_LIMIT),
        interpret=pltpu.InterpretParams() if INTERPRET else False,
    )


VM = pl.BlockSpec(memory_space=pltpu.VMEM)
SM = pl.BlockSpec(memory_space=pltpu.SMEM)
HB = pl.BlockSpec(memory_space=pltpu.HBM)


def call(kernel, name, out_shape, in_specs, scratch=()):
    return pl.pallas_call(
        kernel,
        name=name,
        out_shape=[
            s if isinstance(s, jax.ShapeDtypeStruct) else jax.ShapeDtypeStruct(s, F32)
            for s in out_shape
        ],
        in_specs=in_specs,
        out_specs=[VM] * len(out_shape),
        scratch_shapes=list(scratch),
        **params(),
    )


WORK = [
    pltpu.VMEM((DP, 3 * SP + GP), F32),
    pltpu.VMEM((DP, LB), F32),
    pltpu.VMEM((DP, LB), F32),
]


def first_solver(
    ids, freq, real, imag, weight, coords, pairs, directions, flux, start, points, eigen, basis
):
    def kernel(
        ids, freq, real_h, imag_h, weight_h, coords_h, pairs_h, directions_h, flux_h, start_h,
        points_h, eigen_h, basis_h,
        out, own, eigen_out, basis_out, vis, base, uvw, ants, cols, stations, dirs,
        acc, re_s, im_s, rows, tall, real, imag, weight, coords, pairs, directions, flux, start,
        points, sems,
    ):
        copies = [
            pltpu.make_async_copy(source, target, sems.at[i])
            for i, (source, target) in enumerate(
                (
                    (points_h, points), (start_h, start), (directions_h, directions),
                    (flux_h, flux), (coords_h, coords), (pairs_h, pairs), (real_h, real),
                    (imag_h, imag), (weight_h, weight), (eigen_h, eigen_out),
                    (basis_h, basis_out),
                )
            )
        ]
        for copy in copies:
            copy.start()
        vis[...] = jnp.zeros_like(vis)
        uvw[...] = jnp.zeros_like(uvw)
        base[...] = jnp.zeros_like(base)
        ants[...] = jnp.full(ants.shape, -1, jnp.int32)
        rows[...] = jnp.zeros_like(rows)
        tall[...] = jnp.zeros_like(tall)
        stations[...] = jnp.full(stations.shape, -1, jnp.int32)
        dirs[...] = jnp.full(dirs.shape, -1, jnp.int32)
        for copy in copies[:-2]:
            copy.wait()
        vis[0:1, 0:B] = real[0]
        vis[1:2, 0:B] = imag[0]
        vis[2:3, 0:B] = weight[0]
        ants[:, 0:B] = pairs[...]
        rows[0:1, 0:D] = flux[...]
        cols[...] = jnp.broadcast_to(rows[0:1, :], (128, 256)).T[:DP, :]
        unit = freq[...] * freq[...] * (TWO_PI / TEC_PHASE)
        for c in range(3):
            place_parts = split3(directions[c : c + 1, :])
            coord_parts = split3(coords[c] * unit)
            for j, (m, n) in enumerate(PRODUCTS):
                k = len(PRODUCTS) * c + j
                tall[SP + k : SP + k + 1, 0:D] = place_parts[m]
                uvw[k : k + 1, 0:B] = coord_parts[n]
        for k in range(S):
            tall[k : k + 1, 0:D] = start[k]
        turned = tall[...].T[:DP, :]
        base[:, 3 * SP : 3 * SP + GP] = turned[:, SP : SP + GP]
        q = points[...]
        s = jnp.floor((q.astype(F32) + 0.5) * (1.0 / D)).astype(jnp.int32)
        d = q - s * D
        for c in range(CH):
            stations[c, 0:1, 0:PB] = s[:, c * PB : (c + 1) * PB]
            dirs[c, 0:1, 0:PB] = d[:, c * PB : (c + 1) * PB]
        solver(
            freq, None, vis, None, uvw, ants, cols, stations, dirs, out, (acc, re_s, im_s),
            own=(stacked(turned[:, :SP]), turned[:, SP : SP + GP].astype(BF16), ids[0], own),
        )
        for copy in copies[-2:]:
            copy.wait()

    i32 = lambda *shape: jax.ShapeDtypeStruct(shape, jnp.int32)
    small = [
        pltpu.VMEM(x.shape, x.dtype)
        for x in (real, imag, weight, coords, pairs, directions, flux, start, points)
    ]
    return call(
        kernel,
        "first_solver",
        [
            (CH, 1, 2 * PW), (1, PW), (1, K), (PB, K), (3, BP), (DP, 3 * SP + GP), (GP, BP),
            i32(2, BP), (DP, 128), i32(CH, 1, PW), i32(CH, 1, PW),
        ],
        [SM, VM] + [HB] * 11,
        WORK
        + [pltpu.VMEM((8, 256), F32), pltpu.VMEM((128, 256), F32)]
        + small
        + [pltpu.SemaphoreType.DMA((11,))],
    )(ids, freq, real, imag, weight, coords, pairs, directions, flux, start, points, eigen, basis)


def next_solver(freq, tec, held, last):
    def kernel(freq, tec, vis, base, uvw, ants, cols, stations, dirs, out, *refs):
        if last:
            real, imag, acc, re_s, im_s, left = refs
            kept = (left, real, imag)
        else:
            acc, re_s, im_s = refs
            kept = None
        solver(
            freq, tec, vis, base, uvw, ants, cols, stations, dirs, out, (acc, re_s, im_s),
            kept=kept,
        )

    return call(
        kernel,
        "last_solver" if last else "next_solver",
        [(CH, 1, PW)] + ([(1, 1, B), (1, 1, B)] if last else []),
        [VM] * 9,
        WORK + ([pltpu.VMEM((2, BP), F32)] if last else []),
    )(freq, tec, *held)


def final_place(vals, stations, dirs):
    def kernel(vals, stations, dirs, out, acc):
        acc[...] = jnp.zeros_like(acc)

        def place(i, carry):
            by_station, by_direction = placed_parts(vals, stations, dirs, i)
            acc[...] += dot_nt(by_station, by_direction)
            return carry

        lax.fori_loop(0, CH // NB, place, 0)
        whole = (acc[0:SP, :] + acc[SP : 2 * SP, :]) + acc[2 * SP : 3 * SP, :]
        for k in range(S):
            out[k] = whole[k : k + 1, :D]

    return call(kernel, "final_place", [(S, 1, D)], [VM] * 3, [pltpu.VMEM((3 * SP, DP), F32)])(
        vals, stations, dirs
    )[0]


def own_target(arrived, own, denominator):
    first = denominator is None

    def kernel(arrived, own, *refs):
        total = jnp.sum(arrived[...], axis=0)
        if first:
            out, den_out = refs
            den = total[:, PW:]
            den_out[...] = den
        else:
            den_ref, out = refs
            den = den_ref[...]
        lane = lax.broadcasted_iota(jnp.int32, (1, PW), 1)
        out[...] = jnp.where(lane < PB, own[...] + total[:, :PW] / den, 0.0)

    if first:
        return call(kernel, "own_target_first", [(1, PW), (1, PW)], [VM] * 2)(arrived, own)
    return call(kernel, "own_target", [(1, PW)], [VM] * 3)(arrived, own, denominator)[0], denominator


GROUPS = [(r, min(8, PB - r)) for r in range(0, PB, 8)]


def basis_partial(ids, slots, target, near, far, weight, basis):
    def kernel(ids, target, near, far, weight, basis, out, tall):
        slot = ids[1]
        ends = (slot == 0).astype(F32) + (slot == slots - 1).astype(F32)
        x = (target[...] + SMOOTHING * (near[...] + far[...])) / (1.0 + SMOOTHING * (2.0 - ends))
        tall[...] = jnp.broadcast_to(x, (128, PW)).T
        total = jnp.zeros((8, K), F32)
        for r, m in GROUPS:
            piece = basis[r : r + m, :] * jnp.concatenate([tall[r : r + m, :]] * (K // 128), axis=1)
            if m == 8:
                total = total + piece
        row = jnp.sum(total, axis=0, keepdims=True) + jnp.sum(piece, axis=0, keepdims=True)
        row = row * weight[...]
        for c in range(CH):
            out[c] = row

    return call(
        kernel,
        "basis_partial",
        [(CH, 1, K)],
        [SM] + [VM] * 5,
        [pltpu.VMEM((PW, 128), F32)],
    )(ids, target, near, far, weight, basis)[0]


def own_screen(arrived, basis):
    def kernel(arrived, basis, coef, own, out, tall):
        row = jnp.sum(arrived[...], axis=0)
        coef[...] = row
        spread = jnp.broadcast_to(row, (8, K))
        tall[PW - 16 : PW, :] = jnp.zeros((16, 128), F32)
        for r, m in GROUPS:
            piece = basis[r : r + m, :] * spread[0:m, :]
            parts = [piece[:, k : k + 128] for k in range(0, K, 128)]
            while len(parts) > 1:
                parts = [u + v for u, v in zip(parts[0::2], parts[1::2])]
            tall[r : r + m, :] = parts[0]
        line = jnp.sum(tall[...].T, axis=0, keepdims=True)
        own[...] = line
        for c in range(CH):
            out[c] = line

    return call(
        kernel,
        "own_screen",
        [(1, K), (1, PW), (CH, 1, PW)],
        [VM, VM],
        [pltpu.VMEM((PW, 128), F32)],
    )(arrived, basis)


def exchange(value):
    return lax.all_to_all(value, "chan", split_axis=0, concat_axis=0, tiled=True)


def per_device(
    measured_real,
    measured_imaginary,
    measured_weight,
    baseline_vectors,
    antenna_pairs,
    directions,
    direction_flux,
    channel_frequency,
    electron_content_start,
    pierce_station_direction,
    eigen_basis,
    eigen_weight,
):
    slots = lax.axis_size("slot")
    ids = jnp.stack([lax.axis_index("chan"), lax.axis_index("slot")]).astype(jnp.int32)
    freq = channel_frequency.reshape(1, 1)
    near_pairs = [(i, i ^ 1) for i in range(slots) if i ^ 1 < slots]
    far_pairs = [(i, i - 1 if i % 2 == 0 else i + 1) for i in range(1, slots - 1)]
    far_pairs = [(i, j) for i, j in far_pairs if 0 <= j < slots]
    sent, own, weight, basis, *held = first_solver(
        ids, freq, measured_real, measured_imaginary, measured_weight,
        jnp.transpose(baseline_vectors, (1, 0, 2)), antenna_pairs, directions, direction_flux,
        jnp.transpose(electron_content_start, (1, 0, 2)), pierce_station_direction,
        eigen_weight[None, :], eigen_basis,
    )
    denominator = None
    for iteration in range(ITERS):
        if iteration > 0:
            sent, *left = next_solver(freq, gathered, held, iteration == ITERS - 1)
        target, denominator = own_target(exchange(sent), own, denominator)
        far = lax.ppermute(target, "slot", far_pairs)
        near = lax.ppermute(target, "slot", near_pairs)
        partial = basis_partial(ids, slots, target, near, far, weight, basis)
        coefficients, own, spread = own_screen(exchange(partial), basis)
        gathered = exchange(spread)
    tec_final = jnp.transpose(final_place(gathered, held[-2], held[-1]), (1, 0, 2))
    return tec_final, coefficients, left[0], left[1]


def solution(mesh):
    in_specs = (
        P("slot", "chan", None),
        P("slot", "chan", None),
        P("slot", "chan", None),
        P("slot", None, None),
        P(),
        P(),
        P("chan", None),
        P("chan"),
        P("slot", None, None),
        P("slot", None),
        P("chan", None),
        P(),
    )
    out_specs = (
        P("slot", None, None),
        P("slot", None),
        P("slot", "chan", None),
        P("slot", "chan", None),
    )
    return jax.shard_map(
        per_device, mesh=mesh, in_specs=in_specs, out_specs=out_specs, check_vma=False
    )
```

```python
import jax
import jax.numpy as jnp
from jax import lax
from jax.experimental import pallas as pl
from jax.experimental.pallas import tpu as pltpu
from jax.sharding import PartitionSpec as P

ITERS = 4
TEC_PHASE = -0.8448
SMOOTHING = 0.5
TWO_PI = 6.283185307179586
INTERPRET = False
VMEM_LIMIT = 16 * 1024 * 1024

S, D, K, B = 60, 200, 2048, 1770
SP, DP, BP = 64, 208, 1792
CH, PB, PW = 32, 375, 384
LB = 256
NB = 16
F32, BF16 = jnp.float32, jnp.bfloat16

COS = (1.4142134965650244, -6.978850988240614, 5.7394611707149, -1.883562987515013, 0.3106981922394431)
SIN = (4.4428828341499464, -7.308241154547178, 3.606288958237895, -0.8457635962132565, 0.10920575375700989)

PRODUCTS = ((0, 0), (0, 1), (1, 0), (1, 1), (0, 2), (2, 0))
GP = 32


def horner(coefficients, z):
    value = coefficients[-1] * z + coefficients[-2]
    for term in coefficients[-3::-1]:
        value = value * z + term
    return value


def split3(x):
    high = x.astype(BF16).astype(F32)
    rest = x - high
    middle = rest.astype(BF16).astype(F32)
    return high, middle, rest - middle


def dot_nt(a, b):
    return lax.dot_general(a, b, (((1,), (1,)), ((), ())), preferred_element_type=F32)


def dot_nn(a, b):
    return lax.dot_general(a, b, (((1,), (0,)), ((), ())), preferred_element_type=F32)


def one_hot(numbers, rows):
    return lax.broadcasted_iota(jnp.int32, (rows, numbers.shape[1]), 0) == numbers


def joined(blocks, i):
    return jnp.concatenate([blocks[NB * i + k] for k in range(NB)], axis=1)


def placed_parts(vals, stations, dirs, i):
    v, s, d = joined(vals, i), joined(stations, i), joined(dirs, i)
    at = one_hot(s, SP)
    by_station = jnp.concatenate(
        [jnp.where(at, part, 0.0).astype(BF16) for part in split3(v)], axis=0
    )
    by_direction = jnp.where(one_hot(d, DP), 1.0, 0.0).astype(BF16)
    return by_station, by_direction


def picked(parts, s, d):
    at = jnp.where(one_hot(s, SP), 1.0, 0.0).astype(BF16)
    rows = dot_nn(parts, jnp.concatenate([at, at, at], axis=0))
    return jnp.sum(jnp.where(one_hot(d, DP), rows, 0.0), axis=0, keepdims=True)


def stacked(field):
    return jnp.concatenate([part.astype(BF16) for part in split3(field)], axis=1)


def solver(freq, tec, vis, base, coords, pairs, cols, stations, dirs, out, work, own=None, kept=None):
    acc, re_s, im_s = work
    tec_scale = TEC_PHASE / freq[...]
    turn_scale = jnp.broadcast_to(tec_scale * (1.0 / TWO_PI), (8, 128))
    first = own is not None
    if first:
        tec_parts, base_parts, mine, own_out = own
        own_out[...] = picked(tec_parts, stations[mine], dirs[mine])
        parts = jnp.concatenate([tec_parts, base_parts], axis=1)
    else:
        acc[...] = base[...]

        def place(i, carry):
            by_station, by_direction = placed_parts(tec, stations, dirs, i)
            acc[:, 0 : 3 * SP] += dot_nt(by_direction, by_station)
            return carry

        lax.fori_loop(0, CH // NB, place, 0)
        parts = acc[...].astype(BF16)

    def chunk(j, carry):
        numer, weight_sum = carry
        lanes = pl.ds(j * LB, LB)
        first_at = one_hot(pairs[0:1, lanes], SP)
        second_at = one_hot(pairs[1:2, lanes], SP)
        sign = jnp.where(first_at, 1.0, jnp.where(second_at, -1.0, 0.0)).astype(BF16)
        mixed = dot_nn(
            parts, jnp.concatenate([sign, sign, sign, coords[:, lanes].astype(BF16)], axis=0)
        )
        data = vis[:, lanes]
        sums = []
        for h in range(LB // 128):
            sum_re = jnp.zeros((8, 128), F32)
            sum_im = jnp.zeros((8, 128), F32)
            for g in range(DP // 8):
                rows = slice(8 * g, 8 * g + 8)
                turns = turn_scale * mixed[rows, h * 128 : (h + 1) * 128]
                r = turns - jnp.round(turns)
                z = r * r
                flux = cols[rows, :]
                half_sin = r * horner(SIN, z)
                re = flux - flux * (half_sin * half_sin)
                im = flux * (half_sin * horner(COS, z))
                re_s[rows, h * 128 : (h + 1) * 128] = re
                im_s[rows, h * 128 : (h + 1) * 128] = im
                sum_re = sum_re + re
                sum_im = sum_im + im
            sums.append(
                (jnp.sum(sum_re, axis=0, keepdims=True), jnp.sum(sum_im, axis=0, keepdims=True))
            )
        left_re = data[0:1, :] - jnp.concatenate([a for a, _ in sums], axis=1)
        left_im = data[1:2, :] - jnp.concatenate([b for _, b in sums], axis=1)
        if kept is not None:
            kept[0][0:1, lanes] = left_re
            kept[0][1:2, lanes] = left_im
        weight = data[2:3, :]
        proj = re_s[...] * (weight * left_im) - im_s[...] * (weight * left_re)
        high = proj.astype(BF16)
        low = (proj - high.astype(F32)).astype(BF16)
        numer = numer + (dot_nt(high, sign) + dot_nt(low, sign))
        if first:
            touched = jnp.where(first_at | second_at, weight, 0.0)
            weight_sum = weight_sum + (touched[:, :128] + touched[:, 128:])
        return numer, weight_sum

    numer, weight_sum = jnp.zeros((DP, SP), F32), jnp.zeros((SP, 128), F32)
    for j in range(BP // LB):
        numer, weight_sum = chunk(j, (numer, weight_sum))
    if kept is not None:
        kept[1][0] = kept[0][0:1, 0:B]
        kept[2][0] = kept[0][1:2, 0:B]
    numer_parts = stacked(numer * tec_scale)
    if first:
        weight_at = jnp.sum(weight_sum, axis=1, keepdims=True) * (tec_scale * tec_scale)
        flux_col = cols[:, 0:1]
        flux_col = flux_col * flux_col

    def pick(i, carry):
        s, d = joined(stations, i), joined(dirs, i)
        got = picked(numer_parts, s, d)
        for k in range(NB):
            out[NB * i + k, 0:1, 0:PW] = got[:, k * PW : (k + 1) * PW]
        if first:
            w_at = jnp.sum(jnp.where(one_hot(s, SP), weight_at, 0.0), axis=0, keepdims=True)
            f_at = jnp.sum(jnp.where(one_hot(d, DP), flux_col, 0.0), axis=0, keepdims=True)
            den = w_at * f_at
            for k in range(NB):
                out[NB * i + k, 0:1, PW : 2 * PW] = den[:, k * PW : (k + 1) * PW]
        return carry

    lax.fori_loop(0, CH // NB, pick, 0)


def params():
    return dict(
        compiler_params=pltpu.CompilerParams(vmem_limit_bytes=VMEM_LIMIT),
        interpret=pltpu.InterpretParams() if INTERPRET else False,
    )


VM = pl.BlockSpec(memory_space=pltpu.VMEM)
SM = pl.BlockSpec(memory_space=pltpu.SMEM)
HB = pl.BlockSpec(memory_space=pltpu.HBM)


def call(kernel, name, out_shape, in_specs, scratch=()):
    return pl.pallas_call(
        kernel,
        name=name,
        out_shape=[
            s if isinstance(s, jax.ShapeDtypeStruct) else jax.ShapeDtypeStruct(s, F32)
            for s in out_shape
        ],
        in_specs=in_specs,
        out_specs=[VM] * len(out_shape),
        scratch_shapes=list(scratch),
        **params(),
    )


WORK = [
    pltpu.VMEM((DP, 3 * SP + GP), F32),
    pltpu.VMEM((DP, LB), F32),
    pltpu.VMEM((DP, LB), F32),
]


def first_solver(
    ids, freq, real, imag, weight, coords, pairs, directions, flux, start, points, eigen, basis
):
    def kernel(
        ids, freq, real_h, imag_h, weight_h, coords_h, pairs_h, directions_h, flux_h, start_h,
        points_h, eigen_h, basis_h,
        out, own, eigen_out, basis_out, vis, base, uvw, ants, cols, stations, dirs,
        acc, re_s, im_s, rows, tall, real, imag, weight, coords, pairs, directions, flux, start,
        points, sems,
    ):
        copies = [
            pltpu.make_async_copy(source, target, sems.at[i])
            for i, (source, target) in enumerate(
                (
                    (points_h, points), (start_h, start), (directions_h, directions),
                    (flux_h, flux), (coords_h, coords), (pairs_h, pairs), (real_h, real),
                    (imag_h, imag), (weight_h, weight), (eigen_h, eigen_out),
                    (basis_h, basis_out),
                )
            )
        ]
        for copy in copies:
            copy.start()
        vis[...] = jnp.zeros_like(vis)
        uvw[...] = jnp.zeros_like(uvw)
        base[...] = jnp.zeros_like(base)
        ants[...] = jnp.full(ants.shape, -1, jnp.int32)
        rows[...] = jnp.zeros_like(rows)
        tall[...] = jnp.zeros_like(tall)
        stations[...] = jnp.full(stations.shape, -1, jnp.int32)
        dirs[...] = jnp.full(dirs.shape, -1, jnp.int32)
        for copy in copies[:-2]:
            copy.wait()
        vis[0:1, 0:B] = real[0]
        vis[1:2, 0:B] = imag[0]
        vis[2:3, 0:B] = weight[0]
        ants[:, 0:B] = pairs[...]
        rows[0:1, 0:D] = flux[...]
        cols[...] = jnp.broadcast_to(rows[0:1, :], (128, 256)).T[:DP, :]
        unit = freq[...] * freq[...] * (TWO_PI / TEC_PHASE)
        for c in range(3):
            place_parts = split3(directions[c : c + 1, :])
            coord_parts = split3(coords[c] * unit)
            for j, (m, n) in enumerate(PRODUCTS):
                k = len(PRODUCTS) * c + j
                tall[SP + k : SP + k + 1, 0:D] = place_parts[m]
                uvw[k : k + 1, 0:B] = coord_parts[n]
        for k in range(S):
            tall[k : k + 1, 0:D] = start[k]
        turned = tall[...].T[:DP, :]
        base[:, 3 * SP : 3 * SP + GP] = turned[:, SP : SP + GP]
        q = points[...]
        s = jnp.floor((q.astype(F32) + 0.5) * (1.0 / D)).astype(jnp.int32)
        d = q - s * D
        for c in range(CH):
            stations[c, 0:1, 0:PB] = s[:, c * PB : (c + 1) * PB]
            dirs[c, 0:1, 0:PB] = d[:, c * PB : (c + 1) * PB]
        solver(
            freq, None, vis, None, uvw, ants, cols, stations, dirs, out, (acc, re_s, im_s),
            own=(stacked(turned[:, :SP]), turned[:, SP : SP + GP].astype(BF16), ids[0], own),
        )
        for copy in copies[-2:]:
            copy.wait()

    i32 = lambda *shape: jax.ShapeDtypeStruct(shape, jnp.int32)
    small = [
        pltpu.VMEM(x.shape, x.dtype)
        for x in (real, imag, weight, coords, pairs, directions, flux, start, points)
    ]
    return call(
        kernel,
        "first_solver",
        [
            (CH, 1, 2 * PW), (1, PW), (1, K), (PB, K), (3, BP), (DP, 3 * SP + GP), (GP, BP),
            i32(2, BP), (DP, 128), i32(CH, 1, PW), i32(CH, 1, PW),
        ],
        [SM, VM] + [HB] * 11,
        WORK
        + [pltpu.VMEM((8, 256), F32), pltpu.VMEM((128, 256), F32)]
        + small
        + [pltpu.SemaphoreType.DMA((11,))],
    )(ids, freq, real, imag, weight, coords, pairs, directions, flux, start, points, eigen, basis)


def next_solver(freq, tec, held, last):
    def kernel(freq, tec, vis, base, uvw, ants, cols, stations, dirs, out, *refs):
        if last:
            real, imag, acc, re_s, im_s, left = refs
            kept = (left, real, imag)
        else:
            acc, re_s, im_s = refs
            kept = None
        solver(
            freq, tec, vis, base, uvw, ants, cols, stations, dirs, out, (acc, re_s, im_s),
            kept=kept,
        )

    return call(
        kernel,
        "last_solver" if last else "next_solver",
        [(CH, 1, PW)] + ([(1, 1, B), (1, 1, B)] if last else []),
        [VM] * 9,
        WORK + ([pltpu.VMEM((2, BP), F32)] if last else []),
    )(freq, tec, *held)


def final_place(vals, stations, dirs):
    def kernel(vals, stations, dirs, out, acc):
        acc[...] = jnp.zeros_like(acc)

        def place(i, carry):
            by_station, by_direction = placed_parts(vals, stations, dirs, i)
            acc[...] += dot_nt(by_station, by_direction)
            return carry

        lax.fori_loop(0, CH // NB, place, 0)
        whole = (acc[0:SP, :] + acc[SP : 2 * SP, :]) + acc[2 * SP : 3 * SP, :]
        for k in range(S):
            out[k] = whole[k : k + 1, :D]

    return call(kernel, "final_place", [(S, 1, D)], [VM] * 3, [pltpu.VMEM((3 * SP, DP), F32)])(
        vals, stations, dirs
    )[0]


def own_target(arrived, own, denominator):
    first = denominator is None

    def kernel(arrived, own, *refs):
        total = jnp.sum(arrived[...], axis=0)
        if first:
            out, den_out = refs
            den = total[:, PW:]
            den_out[...] = den
        else:
            den_ref, out = refs
            den = den_ref[...]
        lane = lax.broadcasted_iota(jnp.int32, (1, PW), 1)
        out[...] = jnp.where(lane < PB, own[...] + total[:, :PW] / den, 0.0)

    if first:
        return call(kernel, "own_target_first", [(1, PW), (1, PW)], [VM] * 2)(arrived, own)
    return call(kernel, "own_target", [(1, PW)], [VM] * 3)(arrived, own, denominator)[0], denominator


GROUPS = [(r, min(8, PB - r)) for r in range(0, PB, 8)]


def basis_partial(ids, slots, target, near, far, weight, basis):
    def kernel(ids, target, near, far, weight, basis, out, tall):
        slot = ids[1]
        ends = (slot == 0).astype(F32) + (slot == slots - 1).astype(F32)
        x = (target[...] + SMOOTHING * (near[...] + far[...])) / (1.0 + SMOOTHING * (2.0 - ends))
        tall[...] = jnp.broadcast_to(x, (128, PW)).T
        total = jnp.zeros((8, K), F32)
        for r, m in GROUPS:
            piece = basis[r : r + m, :] * jnp.concatenate([tall[r : r + m, :]] * (K // 128), axis=1)
            if m == 8:
                total = total + piece
        row = jnp.sum(total, axis=0, keepdims=True) + jnp.sum(piece, axis=0, keepdims=True)
        row = row * weight[...]
        for c in range(CH):
            out[c] = row

    return call(
        kernel,
        "basis_partial",
        [(CH, 1, K)],
        [SM] + [VM] * 5,
        [pltpu.VMEM((PW, 128), F32)],
    )(ids, target, near, far, weight, basis)[0]


def own_screen(arrived, basis):
    def kernel(arrived, basis, coef, own, out, tall):
        row = jnp.sum(arrived[...], axis=0)
        coef[...] = row
        spread = jnp.broadcast_to(row, (8, K))
        tall[PW - 16 : PW, :] = jnp.zeros((16, 128), F32)
        for r, m in GROUPS:
            piece = basis[r : r + m, :] * spread[0:m, :]
            parts = [piece[:, k : k + 128] for k in range(0, K, 128)]
            while len(parts) > 1:
                parts = [u + v for u, v in zip(parts[0::2], parts[1::2])]
            tall[r : r + m, :] = parts[0]
        line = jnp.sum(tall[...].T, axis=0, keepdims=True)
        own[...] = line
        for c in range(CH):
            out[c] = line

    return call(
        kernel,
        "own_screen",
        [(1, K), (1, PW), (CH, 1, PW)],
        [VM, VM],
        [pltpu.VMEM((PW, 128), F32)],
    )(arrived, basis)


def exchange(value):
    return lax.all_to_all(value, "chan", split_axis=0, concat_axis=0, tiled=True)


def per_device(
    measured_real,
    measured_imaginary,
    measured_weight,
    baseline_vectors,
    antenna_pairs,
    directions,
    direction_flux,
    channel_frequency,
    electron_content_start,
    pierce_station_direction,
    eigen_basis,
    eigen_weight,
):
    slots = lax.axis_size("slot")
    ids = jnp.stack([lax.axis_index("chan"), lax.axis_index("slot")]).astype(jnp.int32)
    freq = channel_frequency.reshape(1, 1)
    near_pairs = [(i, i ^ 1) for i in range(slots) if i ^ 1 < slots]
    far_pairs = [(i, i - 1 if i % 2 == 0 else i + 1) for i in range(1, slots - 1)]
    far_pairs = [(i, j) for i, j in far_pairs if 0 <= j < slots]
    arguments = [
        pltpu.with_memory_space_constraint(x, pltpu.HBM)
        for x in (
            measured_real, measured_imaginary, measured_weight,
            jnp.transpose(baseline_vectors, (1, 0, 2)), antenna_pairs, directions,
            direction_flux, jnp.transpose(electron_content_start, (1, 0, 2)),
            pierce_station_direction, eigen_weight[None, :], eigen_basis,
        )
    ]
    sent, own, weight, basis, *held = first_solver(ids, freq, *arguments)
    denominator = None
    for iteration in range(ITERS):
        if iteration > 0:
            sent, *left = next_solver(freq, gathered, held, iteration == ITERS - 1)
        target, denominator = own_target(exchange(sent), own, denominator)
        far = lax.ppermute(target, "slot", far_pairs)
        near = lax.ppermute(target, "slot", near_pairs)
        partial = basis_partial(ids, slots, target, near, far, weight, basis)
        coefficients, own, spread = own_screen(exchange(partial), basis)
        gathered = exchange(spread)
    tec_final = jnp.transpose(final_place(gathered, held[-2], held[-1]), (1, 0, 2))
    return tec_final, coefficients, left[0], left[1]


def solution(mesh):
    in_specs = (
        P("slot", "chan", None),
        P("slot", "chan", None),
        P("slot", "chan", None),
        P("slot", None, None),
        P(),
        P(),
        P("chan", None),
        P("chan"),
        P("slot", None, None),
        P("slot", None),
        P("chan", None),
        P(),
    )
    out_specs = (
        P("slot", None, None),
        P("slot", None),
        P("slot", "chan", None),
        P("slot", "chan", None),
    )
    return jax.shard_map(
        per_device, mesh=mesh, in_specs=in_specs, out_specs=out_specs, check_vma=False
    )
```

```python
import jax
import jax.numpy as jnp
from jax import lax
from jax.experimental import pallas as pl
from jax.experimental.pallas import tpu as pltpu
from jax.sharding import PartitionSpec as P

ITERS = 4
TEC_PHASE = -0.8448
SMOOTHING = 0.5
TWO_PI = 6.283185307179586
INTERPRET = False
VMEM_LIMIT = 16 * 1024 * 1024

S, D, K, B = 60, 200, 2048, 1770
SP, DP, BP = 64, 208, 1792
CH, PB, PW = 32, 375, 384
LB = 256
NB = 16
F32, BF16 = jnp.float32, jnp.bfloat16

COS = (1.4142134965650244, -6.978850988240614, 5.7394611707149, -1.883562987515013, 0.3106981922394431)
SIN = (4.4428828341499464, -7.308241154547178, 3.606288958237895, -0.8457635962132565, 0.10920575375700989)

PRODUCTS = ((0, 0), (0, 1), (1, 0), (1, 1), (0, 2), (2, 0))
GP = 32


def horner(coefficients, z):
    value = coefficients[-1] * z + coefficients[-2]
    for term in coefficients[-3::-1]:
        value = value * z + term
    return value


def split3(x):
    high = x.astype(BF16).astype(F32)
    rest = x - high
    middle = rest.astype(BF16).astype(F32)
    return high, middle, rest - middle


def dot_nt(a, b):
    return lax.dot_general(a, b, (((1,), (1,)), ((), ())), preferred_element_type=F32)


def dot_nn(a, b):
    return lax.dot_general(a, b, (((1,), (0,)), ((), ())), preferred_element_type=F32)


def one_hot(numbers, rows):
    return lax.broadcasted_iota(jnp.int32, (rows, numbers.shape[1]), 0) == numbers


def joined(blocks, i):
    return jnp.concatenate([blocks[NB * i + k] for k in range(NB)], axis=1)


def placed_parts(vals, stations, dirs, i):
    v, s, d = joined(vals, i), joined(stations, i), joined(dirs, i)
    at = one_hot(s, SP)
    by_station = jnp.concatenate(
        [jnp.where(at, part, 0.0).astype(BF16) for part in split3(v)], axis=0
    )
    by_direction = jnp.where(one_hot(d, DP), 1.0, 0.0).astype(BF16)
    return by_station, by_direction


def picked(parts, s, d):
    at = jnp.where(one_hot(s, SP), 1.0, 0.0).astype(BF16)
    rows = dot_nn(parts, jnp.concatenate([at, at, at], axis=0))
    ahead = d - lax.broadcasted_iota(jnp.int32, (8, d.shape[1]), 0)
    chosen = jnp.zeros((8, d.shape[1]), F32)
    for g in range(DP // 8):
        chosen = jnp.where(ahead == 8 * g, rows[8 * g : 8 * g + 8, :], chosen)
    return jnp.sum(chosen, axis=0, keepdims=True)


def stacked(field):
    return jnp.concatenate([part.astype(BF16) for part in split3(field)], axis=1)


def solver(freq, tec, vis, base, coords, pairs, cols, stations, dirs, out, work, own=None, kept=None):
    acc, re_s, im_s = work
    tec_scale = TEC_PHASE / freq[...]
    turn_scale = jnp.broadcast_to(tec_scale * (1.0 / TWO_PI), (8, 128))
    first = own is not None
    if first:
        tec_parts, base_parts, flux_row, mine, own_out = own
        own_out[...] = picked(tec_parts, stations[mine], dirs[mine])
        parts = jnp.concatenate([tec_parts, base_parts], axis=1)
    else:
        acc[...] = base[...]

        def place(i, carry):
            by_station, by_direction = placed_parts(tec, stations, dirs, i)
            acc[:, 0 : 3 * SP] += dot_nt(by_direction, by_station)
            return carry

        lax.fori_loop(0, CH // NB, place, 0)
        parts = acc[...].astype(BF16)

    def chunk(j, carry):
        numer, weight_sum = carry
        lanes = pl.ds(j * LB, LB)
        first_at = one_hot(pairs[0:1, lanes], SP)
        second_at = one_hot(pairs[1:2, lanes], SP)
        sign = jnp.where(first_at, 1.0, jnp.where(second_at, -1.0, 0.0)).astype(BF16)
        mixed = dot_nn(
            parts, jnp.concatenate([sign, sign, sign, coords[:, lanes].astype(BF16)], axis=0)
        )
        data = vis[:, lanes]
        sums = []
        for h in range(LB // 128):
            sum_re = jnp.zeros((8, 128), F32)
            sum_im = jnp.zeros((8, 128), F32)
            for g in range(DP // 8):
                rows = slice(8 * g, 8 * g + 8)
                turns = turn_scale * mixed[rows, h * 128 : (h + 1) * 128]
                r = turns - jnp.round(turns)
                z = r * r
                flux = cols[rows, :]
                half_sin = r * horner(SIN, z)
                re = flux - flux * (half_sin * half_sin)
                im = flux * (half_sin * horner(COS, z))
                re_s[rows, h * 128 : (h + 1) * 128] = re
                im_s[rows, h * 128 : (h + 1) * 128] = im
                sum_re = sum_re + re
                sum_im = sum_im + im
            sums.append(
                (jnp.sum(sum_re, axis=0, keepdims=True), jnp.sum(sum_im, axis=0, keepdims=True))
            )
        left_re = data[0:1, :] - jnp.concatenate([a for a, _ in sums], axis=1)
        left_im = data[1:2, :] - jnp.concatenate([b for _, b in sums], axis=1)
        if kept is not None:
            kept[0][0:1, lanes] = left_re
            kept[0][1:2, lanes] = left_im
        weight = data[2:3, :]
        proj = re_s[...] * (weight * left_im) - im_s[...] * (weight * left_re)
        high = proj.astype(BF16)
        low = (proj - high.astype(F32)).astype(BF16)
        numer = numer + (dot_nt(high, sign) + dot_nt(low, sign))
        if first:
            touched = jnp.where(first_at | second_at, weight, 0.0)
            weight_sum = weight_sum + (touched[:, :128] + touched[:, 128:])
        return numer, weight_sum

    numer, weight_sum = jnp.zeros((DP, SP), F32), jnp.zeros((SP, 128), F32)
    for j in range(BP // LB):
        numer, weight_sum = chunk(j, (numer, weight_sum))
    if kept is not None:
        kept[1][0] = kept[0][0:1, 0:B]
        kept[2][0] = kept[0][1:2, 0:B]
    numer_parts = stacked(numer * tec_scale)
    if first:
        weight_tall = jnp.concatenate([weight_sum, jnp.zeros((128 - SP, 128), F32)], axis=0)
        weight_row = jnp.sum(weight_tall.T, axis=0, keepdims=True) * (tec_scale * tec_scale)
        factors = jnp.concatenate([weight_row, flux_row * flux_row], axis=1)

    def pick(i, carry):
        s, d = joined(stations, i), joined(dirs, i)
        got = picked(numer_parts, s, d)
        for k in range(NB):
            out[NB * i + k, 0:1, 0:PW] = got[:, k * PW : (k + 1) * PW]
        if first:
            for k in range(NB):
                out[NB * i + k, 0:1, PW : 2 * PW] = factors
        return carry

    lax.fori_loop(0, CH // NB, pick, 0)


def params():
    return dict(
        compiler_params=pltpu.CompilerParams(vmem_limit_bytes=VMEM_LIMIT),
        interpret=pltpu.InterpretParams() if INTERPRET else False,
    )


VM = pl.BlockSpec(memory_space=pltpu.VMEM)
SM = pl.BlockSpec(memory_space=pltpu.SMEM)
HB = pl.BlockSpec(memory_space=pltpu.HBM)


def call(kernel, name, out_shape, in_specs, scratch=()):
    return pl.pallas_call(
        kernel,
        name=name,
        out_shape=[
            s if isinstance(s, jax.ShapeDtypeStruct) else jax.ShapeDtypeStruct(s, F32)
            for s in out_shape
        ],
        in_specs=in_specs,
        out_specs=[VM] * len(out_shape),
        scratch_shapes=list(scratch),
        **params(),
    )


WORK = [
    pltpu.VMEM((DP, 3 * SP + GP), F32),
    pltpu.VMEM((DP, LB), F32),
    pltpu.VMEM((DP, LB), F32),
]


def first_solver(
    ids, freq, real, imag, weight, coords, pairs, directions, flux, start, points, eigen, basis
):
    def kernel(
        ids, freq, real_h, imag_h, weight_h, coords_h, pairs_h, directions_h, flux_h, start_h,
        points_h, eigen_h, basis_h,
        out, own, eigen_out, basis_out, vis, base, uvw, ants, cols, stations, dirs,
        acc, re_s, im_s, rows, tall, real, imag, weight, coords, pairs, directions, flux, start,
        points, sems,
    ):
        copies = [
            pltpu.make_async_copy(source, target, sems.at[i])
            for i, (source, target) in enumerate(
                (
                    (points_h, points), (start_h, start), (directions_h, directions),
                    (flux_h, flux), (coords_h, coords), (pairs_h, pairs), (real_h, real),
                    (imag_h, imag), (weight_h, weight), (eigen_h, eigen_out),
                    (basis_h, basis_out),
                )
            )
        ]
        for copy in copies:
            copy.start()
        vis[...] = jnp.zeros_like(vis)
        uvw[...] = jnp.zeros_like(uvw)
        base[...] = jnp.zeros_like(base)
        ants[...] = jnp.full(ants.shape, -1, jnp.int32)
        rows[...] = jnp.zeros_like(rows)
        tall[...] = jnp.zeros_like(tall)
        stations[...] = jnp.full(stations.shape, -1, jnp.int32)
        dirs[...] = jnp.full(dirs.shape, -1, jnp.int32)
        for copy in copies[:-2]:
            copy.wait()
        vis[0:1, 0:B] = real[0]
        vis[1:2, 0:B] = imag[0]
        vis[2:3, 0:B] = weight[0]
        ants[:, 0:B] = pairs[...]
        rows[0:1, 0:D] = flux[...]
        cols[...] = jnp.broadcast_to(rows[0:1, :], (128, 256)).T[:DP, :]
        unit = freq[...] * freq[...] * (TWO_PI / TEC_PHASE)
        for c in range(3):
            place_parts = split3(directions[c : c + 1, :])
            coord_parts = split3(coords[c] * unit)
            for j, (m, n) in enumerate(PRODUCTS):
                k = len(PRODUCTS) * c + j
                tall[SP + k : SP + k + 1, 0:D] = place_parts[m]
                uvw[k : k + 1, 0:B] = coord_parts[n]
        for k in range(S):
            tall[k : k + 1, 0:D] = start[k]
        turned = tall[...].T[:DP, :]
        base[:, 3 * SP : 3 * SP + GP] = turned[:, SP : SP + GP]
        q = points[...]
        s = jnp.floor((q.astype(F32) + 0.5) * (1.0 / D)).astype(jnp.int32)
        d = q - s * D
        for c in range(CH):
            stations[c, 0:1, 0:PB] = s[:, c * PB : (c + 1) * PB]
            dirs[c, 0:1, 0:PB] = d[:, c * PB : (c + 1) * PB]
        solver(
            freq, None, vis, None, uvw, ants, cols, stations, dirs, out, (acc, re_s, im_s),
            own=(stacked(turned[:, :SP]), turned[:, SP : SP + GP].astype(BF16),
                 rows[0:1, :], ids[0], own),
        )
        for copy in copies[-2:]:
            copy.wait()

    i32 = lambda *shape: jax.ShapeDtypeStruct(shape, jnp.int32)
    small = [
        pltpu.VMEM(x.shape, x.dtype)
        for x in (real, imag, weight, coords, pairs, directions, flux, start, points)
    ]
    return call(
        kernel,
        "first_solver",
        [
            (CH, 1, 2 * PW), (1, PW), (1, K), (PB, K), (3, BP), (DP, 3 * SP + GP), (GP, BP),
            i32(2, BP), (DP, 128), i32(CH, 1, PW), i32(CH, 1, PW),
        ],
        [SM, VM] + [HB] * 11,
        WORK
        + [pltpu.VMEM((8, 256), F32), pltpu.VMEM((128, 256), F32)]
        + small
        + [pltpu.SemaphoreType.DMA((11,))],
    )(ids, freq, real, imag, weight, coords, pairs, directions, flux, start, points, eigen, basis)


def next_solver(freq, tec, held, last):
    def kernel(freq, tec, vis, base, uvw, ants, cols, stations, dirs, out, *refs):
        if last:
            real, imag, acc, re_s, im_s, left = refs
            kept = (left, real, imag)
        else:
            acc, re_s, im_s = refs
            kept = None
        solver(
            freq, tec, vis, base, uvw, ants, cols, stations, dirs, out, (acc, re_s, im_s),
            kept=kept,
        )

    return call(
        kernel,
        "last_solver" if last else "next_solver",
        [(CH, 1, PW)] + ([(1, 1, B), (1, 1, B)] if last else []),
        [VM] * 9,
        WORK + ([pltpu.VMEM((2, BP), F32)] if last else []),
    )(freq, tec, *held)


def final_place(vals, stations, dirs):
    def kernel(vals, stations, dirs, out, acc):
        acc[...] = jnp.zeros_like(acc)

        def place(i, carry):
            by_station, by_direction = placed_parts(vals, stations, dirs, i)
            acc[...] += dot_nt(by_station, by_direction)
            return carry

        lax.fori_loop(0, CH // NB, place, 0)
        whole = (acc[0:SP, :] + acc[SP : 2 * SP, :]) + acc[2 * SP : 3 * SP, :]
        for k in range(S):
            out[k] = whole[k : k + 1, :D]

    return call(kernel, "final_place", [(S, 1, D)], [VM] * 3, [pltpu.VMEM((3 * SP, DP), F32)])(
        vals, stations, dirs
    )[0]


def own_target_first(ids, arrived, own, stations, dirs):
    def kernel(ids, arrived, own, stations, dirs, out, den_out):
        mine = ids[0]
        factors = jnp.concatenate([arrived[c, 0:1, PW : 2 * PW] for c in range(CH)], axis=0)
        total = jnp.sum(arrived[:, :, 0:PW], axis=0)

        def at_points(field, numbers):
            parts = jnp.concatenate([part.astype(BF16) for part in split3(field)], axis=0)
            hot = jnp.where(one_hot(numbers, field.shape[1]), 1.0, 0.0).astype(BF16)
            found = dot_nn(parts, hot)
            return (found[0:CH] + found[CH : 2 * CH]) + found[2 * CH : 3 * CH]

        weights = at_points(factors[:, 0:128], stations[mine])
        fluxes = at_points(factors[:, 128:384], dirs[mine])
        den = jnp.sum(weights * fluxes, axis=0, keepdims=True)
        den_out[...] = den
        lane = lax.broadcasted_iota(jnp.int32, (1, PW), 1)
        out[...] = jnp.where(lane < PB, own[...] + total / den, 0.0)

    return call(kernel, "own_target_first", [(1, PW), (1, PW)], [SM] + [VM] * 4)(
        ids, arrived, own, stations, dirs
    )


def own_target(arrived, own, denominator):
    def kernel(arrived, own, den, out):
        total = jnp.sum(arrived[...], axis=0)
        lane = lax.broadcasted_iota(jnp.int32, (1, PW), 1)
        out[...] = jnp.where(lane < PB, own[...] + total / den[...], 0.0)

    return call(kernel, "own_target", [(1, PW)], [VM] * 3)(arrived, own, denominator)[0]


GROUPS = [(r, min(8, PB - r)) for r in range(0, PB, 8)]


def basis_partial(ids, slots, target, near, far, weight, basis):
    def kernel(ids, target, near, far, weight, basis, out, tall):
        slot = ids[1]
        ends = (slot == 0).astype(F32) + (slot == slots - 1).astype(F32)
        x = (target[...] + SMOOTHING * (near[...] + far[...])) / (1.0 + SMOOTHING * (2.0 - ends))
        tall[...] = jnp.broadcast_to(x, (128, PW)).T
        total = jnp.zeros((8, K), F32)
        for r, m in GROUPS:
            piece = basis[r : r + m, :] * jnp.concatenate([tall[r : r + m, :]] * (K // 128), axis=1)
            if m == 8:
                total = total + piece
        row = jnp.sum(total, axis=0, keepdims=True) + jnp.sum(piece, axis=0, keepdims=True)
        row = row * weight[...]
        for c in range(CH):
            out[c] = row

    return call(
        kernel,
        "basis_partial",
        [(CH, 1, K)],
        [SM] + [VM] * 5,
        [pltpu.VMEM((PW, 128), F32)],
    )(ids, target, near, far, weight, basis)[0]


def own_screen(arrived, basis):
    def kernel(arrived, basis, coef, own, out, tall):
        row = jnp.sum(arrived[...], axis=0)
        coef[...] = row
        spread = jnp.broadcast_to(row, (8, K))
        tall[PW - 16 : PW, :] = jnp.zeros((16, 128), F32)
        for r, m in GROUPS:
            piece = basis[r : r + m, :] * spread[0:m, :]
            parts = [piece[:, k : k + 128] for k in range(0, K, 128)]
            while len(parts) > 1:
                parts = [u + v for u, v in zip(parts[0::2], parts[1::2])]
            tall[r : r + m, :] = parts[0]
        line = jnp.sum(tall[...].T, axis=0, keepdims=True)
        own[...] = line
        for c in range(CH):
            out[c] = line

    return call(
        kernel,
        "own_screen",
        [(1, K), (1, PW), (CH, 1, PW)],
        [VM, VM],
        [pltpu.VMEM((PW, 128), F32)],
    )(arrived, basis)


def exchange(value):
    return lax.all_to_all(value, "chan", split_axis=0, concat_axis=0, tiled=True)


def per_device(
    measured_real,
    measured_imaginary,
    measured_weight,
    baseline_vectors,
    antenna_pairs,
    directions,
    direction_flux,
    channel_frequency,
    electron_content_start,
    pierce_station_direction,
    eigen_basis,
    eigen_weight,
):
    slots = lax.axis_size("slot")
    ids = jnp.stack([lax.axis_index("chan"), lax.axis_index("slot")]).astype(jnp.int32)
    freq = channel_frequency.reshape(1, 1)
    near_pairs = [(i, i ^ 1) for i in range(slots) if i ^ 1 < slots]
    far_pairs = [(i, i - 1 if i % 2 == 0 else i + 1) for i in range(1, slots - 1)]
    far_pairs = [(i, j) for i, j in far_pairs if 0 <= j < slots]
    arguments = [
        pltpu.with_memory_space_constraint(x, pltpu.HBM)
        for x in (
            measured_real, measured_imaginary, measured_weight,
            jnp.transpose(baseline_vectors, (1, 0, 2)), antenna_pairs, directions,
            direction_flux, jnp.transpose(electron_content_start, (1, 0, 2)),
            pierce_station_direction, eigen_weight[None, :], eigen_basis,
        )
    ]
    sent, own, weight, basis, *held = first_solver(ids, freq, *arguments)
    for iteration in range(ITERS):
        if iteration > 0:
            sent, *left = next_solver(freq, gathered, held, iteration == ITERS - 1)
        if iteration == 0:
            target, denominator = own_target_first(ids, exchange(sent), own, held[-2], held[-1])
        else:
            target = own_target(exchange(sent), own, denominator)
        far = lax.ppermute(target, "slot", far_pairs)
        near = lax.ppermute(target, "slot", near_pairs)
        partial = basis_partial(ids, slots, target, near, far, weight, basis)
        coefficients, own, spread = own_screen(exchange(partial), basis)
        gathered = exchange(spread)
    tec_final = jnp.transpose(final_place(gathered, held[-2], held[-1]), (1, 0, 2))
    return tec_final, coefficients, left[0], left[1]


def solution(mesh):
    in_specs = (
        P("slot", "chan", None),
        P("slot", "chan", None),
        P("slot", "chan", None),
        P("slot", None, None),
        P(),
        P(),
        P("chan", None),
        P("chan"),
        P("slot", None, None),
        P("slot", None),
        P("chan", None),
        P(),
    )
    out_specs = (
        P("slot", None, None),
        P("slot", None),
        P("slot", "chan", None),
        P("slot", "chan", None),
    )
    return jax.shard_map(
        per_device, mesh=mesh, in_specs=in_specs, out_specs=out_specs, check_vma=False
    )
```

```python
import jax
import jax.numpy as jnp
from jax import lax
from jax.experimental import pallas as pl
from jax.experimental.pallas import tpu as pltpu
from jax.sharding import PartitionSpec as P

ITERS = 4
TEC_PHASE = -0.8448
SMOOTHING = 0.5
TWO_PI = 6.283185307179586
INTERPRET = False
VMEM_LIMIT = 16 * 1024 * 1024

S, D, K, B = 60, 200, 2048, 1770
SP, DP, BP = 64, 208, 1792
CH, PB, PW = 32, 375, 384
LB = 256
NB = 16
F32, BF16 = jnp.float32, jnp.bfloat16

COS = (1.4142134965650244, -6.978850988240614, 5.7394611707149, -1.883562987515013, 0.3106981922394431)
SIN = (4.4428828341499464, -7.308241154547178, 3.606288958237895, -0.8457635962132565, 0.10920575375700989)

PRODUCTS = ((0, 0), (0, 1), (1, 0), (1, 1), (0, 2), (2, 0))
GP = 32


def horner(coefficients, z):
    value = coefficients[-1] * z + coefficients[-2]
    for term in coefficients[-3::-1]:
        value = value * z + term
    return value


def split3(x):
    high = x.astype(BF16).astype(F32)
    rest = x - high
    middle = rest.astype(BF16).astype(F32)
    return high, middle, rest - middle


def dot_nt(a, b):
    return lax.dot_general(a, b, (((1,), (1,)), ((), ())), preferred_element_type=F32)


def dot_nn(a, b):
    return lax.dot_general(a, b, (((1,), (0,)), ((), ())), preferred_element_type=F32)


def one_hot(numbers, rows):
    return lax.broadcasted_iota(jnp.int32, (rows, numbers.shape[1]), 0) == numbers


def joined(blocks, i):
    return jnp.concatenate([blocks[NB * i + k] for k in range(NB)], axis=1)


def placed_parts(vals, stations, dirs, i):
    v, s, d = joined(vals, i), joined(stations, i), joined(dirs, i)
    at = one_hot(s, SP)
    by_station = jnp.concatenate(
        [jnp.where(at, part, 0.0).astype(BF16) for part in split3(v)], axis=0
    )
    by_direction = jnp.where(one_hot(d, DP), 1.0, 0.0).astype(BF16)
    return by_station, by_direction


def picked(parts, s, d):
    at = jnp.where(one_hot(s, SP), 1.0, 0.0).astype(BF16)
    rows = dot_nn(parts, jnp.concatenate([at, at, at], axis=0))
    ahead = d - lax.broadcasted_iota(jnp.int32, (8, d.shape[1]), 0)
    chosen = jnp.zeros((8, d.shape[1]), F32)
    for g in range(DP // 8):
        chosen = jnp.where(ahead == 8 * g, rows[8 * g : 8 * g + 8, :], chosen)
    return jnp.sum(chosen, axis=0, keepdims=True)


def stacked(field):
    return jnp.concatenate([part.astype(BF16) for part in split3(field)], axis=1)


def solver(freq, tec, vis, base, coords, pairs, cols, stations, dirs, out, work, own=None, kept=None, ship=None):
    acc, re_s, im_s = work
    tec_scale = TEC_PHASE / freq[...]
    turn_scale = jnp.broadcast_to(tec_scale * (1.0 / TWO_PI), (8, 128))
    first = own is not None
    if first:
        tec_parts, base_parts, flux_row, mine, own_out = own
        own_out[...] = picked(tec_parts, stations[mine], dirs[mine])
        parts = jnp.concatenate([tec_parts, base_parts], axis=1)
    else:
        acc[...] = base[...]

        def place(i, carry):
            by_station, by_direction = placed_parts(tec, stations, dirs, i)
            acc[:, 0 : 3 * SP] += dot_nt(by_direction, by_station)
            return carry

        lax.fori_loop(0, CH // NB, place, 0)
        parts = acc[...].astype(BF16)

    def chunk(j, carry):
        numer, weight_sum = carry
        lanes = pl.ds(j * LB, LB)
        first_at = one_hot(pairs[0:1, lanes], SP)
        second_at = one_hot(pairs[1:2, lanes], SP)
        sign = jnp.where(first_at, 1.0, jnp.where(second_at, -1.0, 0.0)).astype(BF16)
        mixed = dot_nn(
            parts, jnp.concatenate([sign, sign, sign, coords[:, lanes].astype(BF16)], axis=0)
        )
        data = vis[:, lanes]
        sums = []
        for h in range(LB // 128):
            sum_re = jnp.zeros((8, 128), F32)
            sum_im = jnp.zeros((8, 128), F32)
            for g in range(DP // 8):
                rows = slice(8 * g, 8 * g + 8)
                turns = turn_scale * mixed[rows, h * 128 : (h + 1) * 128]
                r = turns - jnp.round(turns)
                z = r * r
                flux = cols[rows, :]
                half_sin = r * horner(SIN, z)
                re = flux - flux * (half_sin * half_sin)
                im = flux * (half_sin * horner(COS, z))
                re_s[rows, h * 128 : (h + 1) * 128] = re
                im_s[rows, h * 128 : (h + 1) * 128] = im
                sum_re = sum_re + re
                sum_im = sum_im + im
            sums.append(
                (jnp.sum(sum_re, axis=0, keepdims=True), jnp.sum(sum_im, axis=0, keepdims=True))
            )
        left_re = data[0:1, :] - jnp.concatenate([a for a, _ in sums], axis=1)
        left_im = data[1:2, :] - jnp.concatenate([b for _, b in sums], axis=1)
        if kept is not None:
            kept[0][0:1, lanes] = left_re
            kept[0][1:2, lanes] = left_im
        weight = data[2:3, :]
        proj = re_s[...] * (weight * left_im) - im_s[...] * (weight * left_re)
        high = proj.astype(BF16)
        low = (proj - high.astype(F32)).astype(BF16)
        numer = numer + (dot_nt(high, sign) + dot_nt(low, sign))
        if first:
            touched = jnp.where(first_at | second_at, weight, 0.0)
            weight_sum = weight_sum + (touched[:, :128] + touched[:, 128:])
        return numer, weight_sum

    numer, weight_sum = jnp.zeros((DP, SP), F32), jnp.zeros((SP, 128), F32)
    for j in range(BP // LB):
        numer, weight_sum = chunk(j, (numer, weight_sum))
    if kept is not None:
        kept[1][0] = kept[0][0:1, 0:B]
        kept[2][0] = kept[0][1:2, 0:B]
    numer_parts = stacked(numer * tec_scale)
    if first:
        weight_tall = jnp.concatenate([weight_sum, jnp.zeros((128 - SP, 128), F32)], axis=0)
        weight_row = jnp.sum(weight_tall.T, axis=0, keepdims=True) * (tec_scale * tec_scale)
        factors = jnp.concatenate([weight_row, flux_row * flux_row], axis=1)

    def pick(i, carry):
        s, d = joined(stations, i), joined(dirs, i)
        got = picked(numer_parts, s, d)
        for k in range(NB):
            for start in (0,) if first else ship[:2]:
                out[start + NB * i + k, 0:1, 0:PW] = got[:, k * PW : (k + 1) * PW]
        if first:
            for k in range(NB):
                out[NB * i + k, 0:1, PW : 2 * PW] = factors
        return carry

    lax.fori_loop(0, CH // NB, pick, 0)
    if not first:
        row = ship[1] + ship[2]
        out[row, 0:1, 0:PW] = out[row, 0:1, 0:PW] + ship[3]


def params():
    return dict(
        compiler_params=pltpu.CompilerParams(vmem_limit_bytes=VMEM_LIMIT),
        interpret=pltpu.InterpretParams() if INTERPRET else False,
    )


VM = pl.BlockSpec(memory_space=pltpu.VMEM)
SM = pl.BlockSpec(memory_space=pltpu.SMEM)
HB = pl.BlockSpec(memory_space=pltpu.HBM)


def call(kernel, name, out_shape, in_specs, scratch=()):
    return pl.pallas_call(
        kernel,
        name=name,
        out_shape=[
            s if isinstance(s, jax.ShapeDtypeStruct) else jax.ShapeDtypeStruct(s, F32)
            for s in out_shape
        ],
        in_specs=in_specs,
        out_specs=[VM] * len(out_shape),
        scratch_shapes=list(scratch),
        **params(),
    )


WORK = [
    pltpu.VMEM((DP, 3 * SP + GP), F32),
    pltpu.VMEM((DP, LB), F32),
    pltpu.VMEM((DP, LB), F32),
]


def first_solver(
    ids, freq, real, imag, weight, coords, pairs, directions, flux, start, points, eigen, basis
):
    def kernel(
        ids, freq, real_h, imag_h, weight_h, coords_h, pairs_h, directions_h, flux_h, start_h,
        points_h, eigen_h, basis_h,
        out, own, eigen_out, basis_out, vis, base, uvw, ants, cols, stations, dirs,
        acc, re_s, im_s, rows, tall, real, imag, weight, coords, pairs, directions, flux, start,
        points, sems,
    ):
        copies = [
            pltpu.make_async_copy(source, target, sems.at[i])
            for i, (source, target) in enumerate(
                (
                    (points_h, points), (start_h, start), (directions_h, directions),
                    (flux_h, flux), (coords_h, coords), (pairs_h, pairs), (real_h, real),
                    (imag_h, imag), (weight_h, weight), (eigen_h, eigen_out),
                    (basis_h, basis_out),
                )
            )
        ]
        for copy in copies:
            copy.start()
        vis[...] = jnp.zeros_like(vis)
        uvw[...] = jnp.zeros_like(uvw)
        base[...] = jnp.zeros_like(base)
        ants[...] = jnp.full(ants.shape, -1, jnp.int32)
        rows[...] = jnp.zeros_like(rows)
        tall[...] = jnp.zeros_like(tall)
        stations[...] = jnp.full(stations.shape, -1, jnp.int32)
        dirs[...] = jnp.full(dirs.shape, -1, jnp.int32)
        for copy in copies[:-2]:
            copy.wait()
        vis[0:1, 0:B] = real[0]
        vis[1:2, 0:B] = imag[0]
        vis[2:3, 0:B] = weight[0]
        ants[:, 0:B] = pairs[...]
        rows[0:1, 0:D] = flux[...]
        cols[...] = jnp.broadcast_to(rows[0:1, :], (128, 256)).T[:DP, :]
        unit = freq[...] * freq[...] * (TWO_PI / TEC_PHASE)
        for c in range(3):
            place_parts = split3(directions[c : c + 1, :])
            coord_parts = split3(coords[c] * unit)
            for j, (m, n) in enumerate(PRODUCTS):
                k = len(PRODUCTS) * c + j
                tall[SP + k : SP + k + 1, 0:D] = place_parts[m]
                uvw[k : k + 1, 0:B] = coord_parts[n]
        for k in range(S):
            tall[k : k + 1, 0:D] = start[k]
        turned = tall[...].T[:DP, :]
        base[:, 3 * SP : 3 * SP + GP] = turned[:, SP : SP + GP]
        q = points[...]
        s = jnp.floor((q.astype(F32) + 0.5) * (1.0 / D)).astype(jnp.int32)
        d = q - s * D
        for c in range(CH):
            stations[c, 0:1, 0:PB] = s[:, c * PB : (c + 1) * PB]
            dirs[c, 0:1, 0:PB] = d[:, c * PB : (c + 1) * PB]
        solver(
            freq, None, vis, None, uvw, ants, cols, stations, dirs, out, (acc, re_s, im_s),
            own=(stacked(turned[:, :SP]), turned[:, SP : SP + GP].astype(BF16),
                 rows[0:1, :], ids[0], own),
        )
        for copy in copies[-2:]:
            copy.wait()

    i32 = lambda *shape: jax.ShapeDtypeStruct(shape, jnp.int32)
    small = [
        pltpu.VMEM(x.shape, x.dtype)
        for x in (real, imag, weight, coords, pairs, directions, flux, start, points)
    ]
    return call(
        kernel,
        "first_solver",
        [
            (CH, 1, 2 * PW), (1, PW), (1, K), (PB, K), (3, BP), (DP, 3 * SP + GP), (GP, BP),
            i32(2, BP), (DP, 128), i32(CH, 1, PW), i32(CH, 1, PW),
        ],
        [SM, VM] + [HB] * 11,
        WORK
        + [pltpu.VMEM((8, 256), F32), pltpu.VMEM((128, 256), F32)]
        + small
        + [pltpu.SemaphoreType.DMA((11,))],
    )(ids, freq, real, imag, weight, coords, pairs, directions, flux, start, points, eigen, basis)


def halves(ids):
    mine = CH * (1 - ids[1] % 2)
    return mine, CH - mine


def next_solver(ids, freq, own, pack, tec, held, last):
    def kernel(ids, freq, own, pack, tec, vis, base, uvw, ants, cols, stations, dirs, out, *refs):
        if last:
            real, imag, acc, re_s, im_s, left = refs
            kept = (left, real, imag)
        else:
            acc, re_s, im_s = refs
            kept = None
        solver(
            freq, tec, vis, base, uvw, ants, cols, stations, dirs, out, (acc, re_s, im_s),
            kept=kept,
            ship=halves(ids) + (ids[0], own[...] * pack[:, PW : 2 * PW]),
        )

    return call(
        kernel,
        "last_solver" if last else "next_solver",
        [(2 * CH, 1, PW)] + ([(1, 1, B), (1, 1, B)] if last else []),
        [SM] + [VM] * 11,
        WORK + ([pltpu.VMEM((2, BP), F32)] if last else []),
    )(ids, freq, own, pack, tec, *held)


def final_place(vals, stations, dirs):
    def kernel(vals, stations, dirs, out, acc):
        acc[...] = jnp.zeros_like(acc)

        def place(i, carry):
            by_station, by_direction = placed_parts(vals, stations, dirs, i)
            acc[...] += dot_nt(by_station, by_direction)
            return carry

        lax.fori_loop(0, CH // NB, place, 0)
        whole = (acc[0:SP, :] + acc[SP : 2 * SP, :]) + acc[2 * SP : 3 * SP, :]
        for k in range(S):
            out[k] = whole[k : k + 1, :D]

    return call(kernel, "final_place", [(S, 1, D)], [VM] * 3, [pltpu.VMEM((3 * SP, DP), F32)])(
        vals, stations, dirs
    )[0]


def own_target_first(ids, arrived, own, stations, dirs):
    def kernel(ids, arrived, own, stations, dirs, out):
        mine = ids[0]
        factors = jnp.concatenate([arrived[c, 0:1, PW : 2 * PW] for c in range(CH)], axis=0)
        total = jnp.sum(arrived[:, :, 0:PW], axis=0)

        def at_points(field, numbers):
            parts = jnp.concatenate([part.astype(BF16) for part in split3(field)], axis=0)
            hot = jnp.where(one_hot(numbers, field.shape[1]), 1.0, 0.0).astype(BF16)
            found = dot_nn(parts, hot)
            return (found[0:CH] + found[CH : 2 * CH]) + found[2 * CH : 3 * CH]

        weights = at_points(factors[:, 0:128], stations[mine])
        fluxes = at_points(factors[:, 128:384], dirs[mine])
        den = jnp.sum(weights * fluxes, axis=0, keepdims=True)
        out[:, PW : 2 * PW] = den
        lane = lax.broadcasted_iota(jnp.int32, (1, PW), 1)
        out[:, 0:PW] = jnp.where(lane < PB, own[...] + total / den, 0.0)

    return call(kernel, "own_target_first", [(1, 2 * PW)], [SM] + [VM] * 4)(
        ids, arrived, own, stations, dirs
    )[0]


def own_target(ids, slots, arrived, own, pack, far_pack):
    def kernel(ids, arrived, own, pack, far_pack, out, far_out):
        mine, pair = halves(ids)
        total = jnp.sum(arrived[pl.ds(mine, CH)], axis=0)
        far = jnp.sum(arrived[pl.ds(pair, CH)], axis=0)
        lane = lax.broadcasted_iota(jnp.int32, (1, PW), 1)
        inner = (ids[1] > 0) & (ids[1] < slots - 1)
        out[...] = jnp.where(lane < PB, own[...] + total / pack[:, PW : 2 * PW], 0.0)
        ends = jnp.where(inner, PB, 0)
        far_out[...] = jnp.where(lane < ends, far / far_pack[:, PW : 2 * PW], 0.0)

    return call(kernel, "own_target", [(1, PW), (1, PW)], [SM] + [VM] * 4)(
        ids, arrived, own, pack, far_pack
    )


GROUPS = [(r, min(8, PB - r)) for r in range(0, PB, 8)]


def basis_partial(ids, slots, target, near, far, weight, basis):
    def kernel(ids, target, near, far, weight, basis, out, tall):
        slot = ids[1]
        ends = (slot == 0).astype(F32) + (slot == slots - 1).astype(F32)
        x = (target[:, 0:PW] + SMOOTHING * (near[:, 0:PW] + far[:, 0:PW])) / (1.0 + SMOOTHING * (2.0 - ends))
        tall[...] = jnp.broadcast_to(x, (128, PW)).T
        total = jnp.zeros((8, K), F32)
        for r, m in GROUPS:
            piece = basis[r : r + m, :] * jnp.concatenate([tall[r : r + m, :]] * (K // 128), axis=1)
            if m == 8:
                total = total + piece
        row = jnp.sum(total, axis=0, keepdims=True) + jnp.sum(piece, axis=0, keepdims=True)
        row = row * weight[...]
        for c in range(CH):
            out[c] = row

    return call(
        kernel,
        "basis_partial",
        [(CH, 1, K)],
        [SM] + [VM] * 5,
        [pltpu.VMEM((PW, 128), F32)],
    )(ids, target, near, far, weight, basis)[0]


def own_screen(arrived, basis):
    def kernel(arrived, basis, coef, own, out, tall):
        row = jnp.sum(arrived[...], axis=0)
        coef[...] = row
        spread = jnp.broadcast_to(row, (8, K))
        tall[PW - 16 : PW, :] = jnp.zeros((16, 128), F32)
        for r, m in GROUPS:
            piece = basis[r : r + m, :] * spread[0:m, :]
            parts = [piece[:, k : k + 128] for k in range(0, K, 128)]
            while len(parts) > 1:
                parts = [u + v for u, v in zip(parts[0::2], parts[1::2])]
            tall[r : r + m, :] = parts[0]
        line = jnp.sum(tall[...].T, axis=0, keepdims=True)
        own[...] = line
        for c in range(CH):
            out[c] = line

    return call(
        kernel,
        "own_screen",
        [(1, K), (1, PW), (CH, 1, PW)],
        [VM, VM],
        [pltpu.VMEM((PW, 128), F32)],
    )(arrived, basis)


def exchange(value):
    return lax.all_to_all(value, "chan", split_axis=0, concat_axis=0, tiled=True)


def per_device(
    measured_real,
    measured_imaginary,
    measured_weight,
    baseline_vectors,
    antenna_pairs,
    directions,
    direction_flux,
    channel_frequency,
    electron_content_start,
    pierce_station_direction,
    eigen_basis,
    eigen_weight,
):
    slots = lax.axis_size("slot")
    ids = jnp.stack([lax.axis_index("chan"), lax.axis_index("slot")]).astype(jnp.int32)
    freq = channel_frequency.reshape(1, 1)
    near_pairs = [(i, i ^ 1) for i in range(slots) if i ^ 1 < slots]
    far_pairs = [(i, i - 1 if i % 2 == 0 else i + 1) for i in range(1, slots - 1)]
    far_pairs = [(i, j) for i, j in far_pairs if 0 <= j < slots]
    arguments = [
        pltpu.with_memory_space_constraint(x, pltpu.HBM)
        for x in (
            measured_real, measured_imaginary, measured_weight,
            jnp.transpose(baseline_vectors, (1, 0, 2)), antenna_pairs, directions,
            direction_flux, jnp.transpose(electron_content_start, (1, 0, 2)),
            pierce_station_direction, eigen_weight[None, :], eigen_basis,
        )
    ]
    sent, own, weight, basis, *held = first_solver(ids, freq, *arguments)
    pair_groups = [
        [c * slots + t for t in (i, (i + 1) % slots) for c in range(CH)]
        for i in range(1, slots, 2)
    ]
    for iteration in range(ITERS):
        if iteration == 0:
            pack = own_target_first(ids, exchange(sent), own, held[-2], held[-1])
            target = pack
            far = far_pack = lax.ppermute(pack, "slot", far_pairs)
        else:
            sent, *left = next_solver(ids, freq, own, pack, gathered, held, iteration == ITERS - 1)
            arrived = lax.all_to_all(
                sent, ("chan", "slot"), 0, 0, tiled=True, axis_index_groups=pair_groups
            )
            target, far = own_target(ids, slots, arrived, own, pack, far_pack)
        near = lax.ppermute(target, "slot", near_pairs)
        partial = basis_partial(ids, slots, target, near, far, weight, basis)
        coefficients, own, spread = own_screen(exchange(partial), basis)
        gathered = exchange(spread)
    tec_final = jnp.transpose(final_place(gathered, held[-2], held[-1]), (1, 0, 2))
    return tec_final, coefficients, left[0], left[1]


def solution(mesh):
    in_specs = (
        P("slot", "chan", None),
        P("slot", "chan", None),
        P("slot", "chan", None),
        P("slot", None, None),
        P(),
        P(),
        P("chan", None),
        P("chan"),
        P("slot", None, None),
        P("slot", None),
        P("chan", None),
        P(),
    )
    out_specs = (
        P("slot", None, None),
        P("slot", None),
        P("slot", "chan", None),
        P("slot", "chan", None),
    )
    return jax.shard_map(
        per_device, mesh=mesh, in_specs=in_specs, out_specs=out_specs, check_vma=False
    )
```

```python
import jax
import jax.numpy as jnp
from jax import lax
from jax.experimental import pallas as pl
from jax.experimental.pallas import tpu as pltpu
from jax.sharding import PartitionSpec as P

ITERS = 4
TEC_PHASE = -0.8448
SMOOTHING = 0.5
TWO_PI = 6.283185307179586
INTERPRET = False
VMEM_LIMIT = 16 * 1024 * 1024

S, D, K, B = 60, 200, 2048, 1770
SP, DP, BP = 64, 208, 1792
CH, PB, PW = 32, 375, 384
LB = 256
NB = 16
F32, BF16 = jnp.float32, jnp.bfloat16

COS = (1.4142134965650244, -6.978850988240614, 5.7394611707149, -1.883562987515013, 0.3106981922394431)
SIN = (4.4428828341499464, -7.308241154547178, 3.606288958237895, -0.8457635962132565, 0.10920575375700989)

PRODUCTS = ((0, 0), (0, 1), (1, 0), (1, 1), (0, 2), (2, 0))
GP = 32


def horner(coefficients, z):
    value = coefficients[-1] * z + coefficients[-2]
    for term in coefficients[-3::-1]:
        value = value * z + term
    return value


def split3(x):
    high = x.astype(BF16).astype(F32)
    rest = x - high
    middle = rest.astype(BF16).astype(F32)
    return high, middle, rest - middle


def dot_nt(a, b):
    return lax.dot_general(a, b, (((1,), (1,)), ((), ())), preferred_element_type=F32)


def dot_nn(a, b):
    return lax.dot_general(a, b, (((1,), (0,)), ((), ())), preferred_element_type=F32)


def one_hot(numbers, rows):
    return lax.broadcasted_iota(jnp.int32, (rows, numbers.shape[1]), 0) == numbers


def joined(blocks, i):
    return jnp.concatenate([blocks[NB * i + k] for k in range(NB)], axis=1)


def placed_parts(vals, stations, dirs, i):
    v, s, d = joined(vals, i), joined(stations, i), joined(dirs, i)
    at = one_hot(s, SP)
    by_station = jnp.concatenate(
        [jnp.where(at, part, 0.0).astype(BF16) for part in split3(v)], axis=0
    )
    by_direction = jnp.where(one_hot(d, DP), 1.0, 0.0).astype(BF16)
    return by_station, by_direction


def picked(parts, s, d):
    at = jnp.where(one_hot(s, SP), 1.0, 0.0).astype(BF16)
    rows = dot_nn(parts, jnp.concatenate([at, at, at], axis=0))
    ahead = d - lax.broadcasted_iota(jnp.int32, (8, d.shape[1]), 0)
    chosen = jnp.zeros((8, d.shape[1]), F32)
    for g in range(D // 8):
        chosen = jnp.where(ahead == 8 * g, rows[8 * g : 8 * g + 8, :], chosen)
    return jnp.sum(chosen, axis=0, keepdims=True)


def stacked(field):
    return jnp.concatenate([part.astype(BF16) for part in split3(field)], axis=1)


def solver(freq, tec, vis, base, coords, pairs, cols, stations, dirs, out, work, own=None, kept=None):
    acc, re_s, im_s = work
    tec_scale = TEC_PHASE / freq[...]
    turn_scale = jnp.broadcast_to(tec_scale * (1.0 / TWO_PI), (8, 128))
    re_s[D:DP, :] = jnp.zeros((DP - D, LB), F32)
    im_s[D:DP, :] = jnp.zeros((DP - D, LB), F32)
    first = own is not None
    if first:
        tec_parts, base_parts, flux_row, mine, own_out = own
        own_out[...] = picked(tec_parts, stations[mine], dirs[mine])
        parts = jnp.concatenate([tec_parts, base_parts], axis=1)
    else:
        acc[...] = base[...]

        def place(i, carry):
            by_station, by_direction = placed_parts(tec, stations, dirs, i)
            acc[:, 0 : 3 * SP] += dot_nt(by_direction, by_station)
            return carry

        lax.fori_loop(0, CH // NB, place, 0)
        parts = acc[...].astype(BF16)

    def chunk(j, carry):
        numer, weight_sum = carry
        lanes = pl.ds(j * LB, LB)
        first_at = one_hot(pairs[0:1, lanes], SP)
        second_at = one_hot(pairs[1:2, lanes], SP)
        sign = jnp.where(first_at, 1.0, jnp.where(second_at, -1.0, 0.0)).astype(BF16)
        mixed = dot_nn(
            parts, jnp.concatenate([sign, sign, sign, coords[:, lanes].astype(BF16)], axis=0)
        )
        data = vis[:, lanes]
        sums = []
        for h in range(LB // 128):
            sum_re = jnp.zeros((8, 128), F32)
            sum_im = jnp.zeros((8, 128), F32)
            for g in range(D // 8):
                rows = slice(8 * g, 8 * g + 8)
                turns = turn_scale * mixed[rows, h * 128 : (h + 1) * 128]
                r = turns - jnp.round(turns)
                z = r * r
                flux = cols[rows, :]
                half_sin = r * horner(SIN, z)
                re = flux - flux * (half_sin * half_sin)
                im = flux * (half_sin * horner(COS, z))
                re_s[rows, h * 128 : (h + 1) * 128] = re
                im_s[rows, h * 128 : (h + 1) * 128] = im
                sum_re = sum_re + re
                sum_im = sum_im + im
            sums.append(
                (jnp.sum(sum_re, axis=0, keepdims=True), jnp.sum(sum_im, axis=0, keepdims=True))
            )
        left_re = data[0:1, :] - jnp.concatenate([a for a, _ in sums], axis=1)
        left_im = data[1:2, :] - jnp.concatenate([b for _, b in sums], axis=1)
        if kept is not None:
            kept[0][0:1, lanes] = left_re
            kept[0][1:2, lanes] = left_im
        weight = data[2:3, :]
        proj = re_s[...] * (weight * left_im) - im_s[...] * (weight * left_re)
        high = proj.astype(BF16)
        low = (proj - high.astype(F32)).astype(BF16)
        numer = numer + (dot_nt(high, sign) + dot_nt(low, sign))
        if first:
            touched = jnp.where(first_at | second_at, weight, 0.0)
            weight_sum = weight_sum + (touched[:, :128] + touched[:, 128:])
        return numer, weight_sum

    numer, weight_sum = jnp.zeros((DP, SP), F32), jnp.zeros((SP, 128), F32)
    for j in range(BP // LB):
        numer, weight_sum = chunk(j, (numer, weight_sum))
    if kept is not None:
        kept[1][0] = kept[0][0:1, 0:B]
        kept[2][0] = kept[0][1:2, 0:B]
    numer_parts = stacked(numer * tec_scale)
    if first:
        weight_tall = jnp.concatenate([weight_sum, jnp.zeros((128 - SP, 128), F32)], axis=0)
        weight_row = jnp.sum(weight_tall.T, axis=0, keepdims=True) * (tec_scale * tec_scale)
        factors = jnp.concatenate([weight_row, flux_row * flux_row], axis=1)

    def pick(i, carry):
        s, d = joined(stations, i), joined(dirs, i)
        got = picked(numer_parts, s, d)
        for k in range(NB):
            out[NB * i + k, 0:1, 0:PW] = got[:, k * PW : (k + 1) * PW]
        if first:
            for k in range(NB):
                out[NB * i + k, 0:1, PW : 2 * PW] = factors
        return carry

    lax.fori_loop(0, CH // NB, pick, 0)


def params():
    return dict(
        compiler_params=pltpu.CompilerParams(vmem_limit_bytes=VMEM_LIMIT),
        interpret=pltpu.InterpretParams() if INTERPRET else False,
    )


VM = pl.BlockSpec(memory_space=pltpu.VMEM)
SM = pl.BlockSpec(memory_space=pltpu.SMEM)
HB = pl.BlockSpec(memory_space=pltpu.HBM)


def call(kernel, name, out_shape, in_specs, scratch=()):
    return pl.pallas_call(
        kernel,
        name=name,
        out_shape=[
            s if isinstance(s, jax.ShapeDtypeStruct) else jax.ShapeDtypeStruct(s, F32)
            for s in out_shape
        ],
        in_specs=in_specs,
        out_specs=[VM] * len(out_shape),
        scratch_shapes=list(scratch),
        **params(),
    )


WORK = [
    pltpu.VMEM((DP, 3 * SP + GP), F32),
    pltpu.VMEM((DP, LB), F32),
    pltpu.VMEM((DP, LB), F32),
]


def first_solver(
    ids, freq, real, imag, weight, coords, pairs, directions, flux, start, points, eigen, basis
):
    def kernel(
        ids, freq, real_h, imag_h, weight_h, coords_h, pairs_h, directions_h, flux_h, start_h,
        points_h, eigen_h, basis_h,
        out, own, eigen_out, basis_out, vis, base, uvw, ants, cols, stations, dirs,
        acc, re_s, im_s, rows, tall, real, imag, weight, coords, pairs, directions, flux, start,
        points, sems,
    ):
        copies = [
            pltpu.make_async_copy(source, target, sems.at[i])
            for i, (source, target) in enumerate(
                (
                    (points_h, points), (start_h, start), (directions_h, directions),
                    (flux_h, flux), (coords_h, coords), (pairs_h, pairs), (real_h, real),
                    (imag_h, imag), (weight_h, weight), (eigen_h, eigen_out),
                    (basis_h, basis_out),
                )
            )
        ]
        for copy in copies:
            copy.start()
        vis[...] = jnp.zeros_like(vis)
        uvw[...] = jnp.zeros_like(uvw)
        base[...] = jnp.zeros_like(base)
        ants[...] = jnp.full(ants.shape, -1, jnp.int32)
        rows[...] = jnp.zeros_like(rows)
        tall[...] = jnp.zeros_like(tall)
        stations[...] = jnp.full(stations.shape, -1, jnp.int32)
        dirs[...] = jnp.full(dirs.shape, -1, jnp.int32)
        for copy in copies[:-2]:
            copy.wait()
        vis[0:1, 0:B] = real[0]
        vis[1:2, 0:B] = imag[0]
        vis[2:3, 0:B] = weight[0]
        ants[:, 0:B] = pairs[...]
        rows[0:1, 0:D] = flux[...]
        cols[...] = jnp.broadcast_to(rows[0:1, :], (128, 256)).T[:DP, :]
        unit = freq[...] * freq[...] * (TWO_PI / TEC_PHASE)
        for c in range(3):
            place_parts = split3(directions[c : c + 1, :])
            coord_parts = split3(coords[c] * unit)
            for j, (m, n) in enumerate(PRODUCTS):
                k = len(PRODUCTS) * c + j
                tall[SP + k : SP + k + 1, 0:D] = place_parts[m]
                uvw[k : k + 1, 0:B] = coord_parts[n]
        for k in range(S):
            tall[k : k + 1, 0:D] = start[k]
        turned = tall[...].T[:DP, :]
        base[:, 3 * SP : 3 * SP + GP] = turned[:, SP : SP + GP]
        q = points[...]
        s = jnp.floor((q.astype(F32) + 0.5) * (1.0 / D)).astype(jnp.int32)
        d = q - s * D
        for c in range(CH):
            stations[c, 0:1, 0:PB] = s[:, c * PB : (c + 1) * PB]
            dirs[c, 0:1, 0:PB] = d[:, c * PB : (c + 1) * PB]
        solver(
            freq, None, vis, None, uvw, ants, cols, stations, dirs, out, (acc, re_s, im_s),
            own=(stacked(turned[:, :SP]), turned[:, SP : SP + GP].astype(BF16),
                 rows[0:1, :], ids[0], own),
        )
        for copy in copies[-2:]:
            copy.wait()

    i32 = lambda *shape: jax.ShapeDtypeStruct(shape, jnp.int32)
    small = [
        pltpu.VMEM(x.shape, x.dtype)
        for x in (real, imag, weight, coords, pairs, directions, flux, start, points)
    ]
    return call(
        kernel,
        "first_solver",
        [
            (CH, 1, 2 * PW), (1, PW), (1, K), (PB, K), (3, BP), (DP, 3 * SP + GP), (GP, BP),
            i32(2, BP), (DP, 128), i32(CH, 1, PW), i32(CH, 1, PW),
        ],
        [SM, VM] + [HB] * 11,
        WORK
        + [pltpu.VMEM((8, 256), F32), pltpu.VMEM((128, 256), F32)]
        + small
        + [pltpu.SemaphoreType.DMA((11,))],
    )(ids, freq, real, imag, weight, coords, pairs, directions, flux, start, points, eigen, basis)


def next_solver(freq, tec, held, last):
    def kernel(freq, tec, vis, base, uvw, ants, cols, stations, dirs, out, *refs):
        if last:
            real, imag, acc, re_s, im_s, left = refs
            kept = (left, real, imag)
        else:
            acc, re_s, im_s = refs
            kept = None
        solver(
            freq, tec, vis, base, uvw, ants, cols, stations, dirs, out, (acc, re_s, im_s),
            kept=kept,
        )

    return call(
        kernel,
        "last_solver" if last else "next_solver",
        [(CH, 1, PW)] + ([(1, 1, B), (1, 1, B)] if last else []),
        [VM] * 9,
        WORK + ([pltpu.VMEM((2, BP), F32)] if last else []),
    )(freq, tec, *held)


def final_place(vals, stations, dirs):
    def kernel(vals, stations, dirs, out, acc):
        acc[...] = jnp.zeros_like(acc)

        def place(i, carry):
            by_station, by_direction = placed_parts(vals, stations, dirs, i)
            acc[...] += dot_nt(by_station, by_direction)
            return carry

        lax.fori_loop(0, CH // NB, place, 0)
        whole = (acc[0:SP, :] + acc[SP : 2 * SP, :]) + acc[2 * SP : 3 * SP, :]
        for k in range(S):
            out[k] = whole[k : k + 1, :D]

    return call(kernel, "final_place", [(S, 1, D)], [VM] * 3, [pltpu.VMEM((3 * SP, DP), F32)])(
        vals, stations, dirs
    )[0]


def own_target_first(ids, arrived, own, stations, dirs):
    def kernel(ids, arrived, own, stations, dirs, out, den_out):
        mine = ids[0]
        factors = jnp.concatenate([arrived[c, 0:1, PW : 2 * PW] for c in range(CH)], axis=0)
        total = jnp.sum(arrived[:, :, 0:PW], axis=0)

        def at_points(field, numbers):
            parts = jnp.concatenate([part.astype(BF16) for part in split3(field)], axis=0)
            hot = jnp.where(one_hot(numbers, field.shape[1]), 1.0, 0.0).astype(BF16)
            found = dot_nn(parts, hot)
            return (found[0:CH] + found[CH : 2 * CH]) + found[2 * CH : 3 * CH]

        weights = at_points(factors[:, 0:128], stations[mine])
        fluxes = at_points(factors[:, 128:384], dirs[mine])
        den = jnp.sum(weights * fluxes, axis=0, keepdims=True)
        den_out[...] = den
        lane = lax.broadcasted_iota(jnp.int32, (1, PW), 1)
        out[...] = jnp.where(lane < PB, own[...] + total / den, 0.0)

    return call(kernel, "own_target_first", [(1, PW), (1, PW)], [SM] + [VM] * 4)(
        ids, arrived, own, stations, dirs
    )


def own_target(arrived, own, denominator):
    def kernel(arrived, own, den, out):
        total = jnp.sum(arrived[...], axis=0)
        lane = lax.broadcasted_iota(jnp.int32, (1, PW), 1)
        out[...] = jnp.where(lane < PB, own[...] + total / den[...], 0.0)

    return call(kernel, "own_target", [(1, PW)], [VM] * 3)(arrived, own, denominator)[0]


GROUPS = [(r, min(8, PB - r)) for r in range(0, PB, 8)]


def basis_partial(ids, slots, target, near, far, weight, basis):
    def kernel(ids, target, near, far, weight, basis, out, tall):
        slot = ids[1]
        ends = (slot == 0).astype(F32) + (slot == slots - 1).astype(F32)
        x = (target[...] + SMOOTHING * (near[...] + far[...])) / (1.0 + SMOOTHING * (2.0 - ends))
        tall[...] = jnp.broadcast_to(x, (128, PW)).T
        total = jnp.zeros((8, K), F32)
        for r, m in GROUPS:
            piece = basis[r : r + m, :] * jnp.concatenate([tall[r : r + m, :]] * (K // 128), axis=1)
            if m == 8:
                total = total + piece
        row = jnp.sum(total, axis=0, keepdims=True) + jnp.sum(piece, axis=0, keepdims=True)
        row = row * weight[...]
        tile = jnp.concatenate([row[:, k : k + 128] for k in range(0, K, 128)], axis=0)
        for c in range(CH):
            out[c] = tile

    return call(
        kernel,
        "basis_partial",
        [(CH, K // 128, 128)],
        [SM] + [VM] * 5,
        [pltpu.VMEM((PW, 128), F32)],
    )(ids, target, near, far, weight, basis)[0]


def own_screen(arrived, basis):
    def kernel(arrived, basis, coef, own, out, tall):
        tile = jnp.sum(arrived[...], axis=0)
        coef[...] = tile
        spread = [jnp.broadcast_to(tile[k : k + 1, :], (8, 128)) for k in range(K // 128)]
        tall[PW - 16 : PW, :] = jnp.zeros((16, 128), F32)
        for r, m in GROUPS:
            parts = [
                basis[r : r + m, 128 * k : 128 * k + 128] * part[0:m, :]
                for k, part in enumerate(spread)
            ]
            while len(parts) > 1:
                parts = [u + v for u, v in zip(parts[0::2], parts[1::2])]
            tall[r : r + m, :] = parts[0]
        line = jnp.sum(tall[...].T, axis=0, keepdims=True)
        own[...] = line
        for c in range(CH):
            out[c] = line

    return call(
        kernel,
        "own_screen",
        [(K // 128, 128), (1, PW), (CH, 1, PW)],
        [VM, VM],
        [pltpu.VMEM((PW, 128), F32)],
    )(arrived, basis)


def exchange(value):
    return lax.all_to_all(value, "chan", split_axis=0, concat_axis=0, tiled=True)


def per_device(
    measured_real,
    measured_imaginary,
    measured_weight,
    baseline_vectors,
    antenna_pairs,
    directions,
    direction_flux,
    channel_frequency,
    electron_content_start,
    pierce_station_direction,
    eigen_basis,
    eigen_weight,
):
    slots = lax.axis_size("slot")
    ids = jnp.stack([lax.axis_index("chan"), lax.axis_index("slot")]).astype(jnp.int32)
    freq = channel_frequency.reshape(1, 1)
    near_pairs = [(i, i ^ 1) for i in range(slots) if i ^ 1 < slots]
    far_pairs = [(i, i - 1 if i % 2 == 0 else i + 1) for i in range(1, slots - 1)]
    far_pairs = [(i, j) for i, j in far_pairs if 0 <= j < slots]
    arguments = [
        pltpu.with_memory_space_constraint(x, pltpu.HBM)
        for x in (
            measured_real, measured_imaginary, measured_weight,
            jnp.transpose(baseline_vectors, (1, 0, 2)), antenna_pairs, directions,
            direction_flux, jnp.transpose(electron_content_start, (1, 0, 2)),
            pierce_station_direction, eigen_weight[None, :], eigen_basis,
        )
    ]
    sent, own, weight, basis, *held = first_solver(ids, freq, *arguments)
    for iteration in range(ITERS):
        if iteration > 0:
            sent, *left = next_solver(freq, gathered, held, iteration == ITERS - 1)
        if iteration == 0:
            target, denominator = own_target_first(ids, exchange(sent), own, held[-2], held[-1])
        else:
            target = own_target(exchange(sent), own, denominator)
        far = lax.ppermute(target, "slot", far_pairs)
        near = lax.ppermute(target, "slot", near_pairs)
        partial = basis_partial(ids, slots, target, near, far, weight, basis)
        coefficients, own, spread = own_screen(exchange(partial), basis)
        gathered = exchange(spread)
    tec_final = jnp.transpose(final_place(gathered, held[-2], held[-1]), (1, 0, 2))
    return tec_final, coefficients.reshape(1, K), left[0], left[1]


def solution(mesh):
    in_specs = (
        P("slot", "chan", None),
        P("slot", "chan", None),
        P("slot", "chan", None),
        P("slot", None, None),
        P(),
        P(),
        P("chan", None),
        P("chan"),
        P("slot", None, None),
        P("slot", None),
        P("chan", None),
        P(),
    )
    out_specs = (
        P("slot", None, None),
        P("slot", None),
        P("slot", "chan", None),
        P("slot", "chan", None),
    )
    return jax.shard_map(
        per_device, mesh=mesh, in_specs=in_specs, out_specs=out_specs, check_vma=False
    )
```
